256 devices in a mesh: rep: 32 (over x, y, core), head: 8 (over z).
Axes of the slice: x: 4, y: 4, z: 8, core: 2. Of those that a mesh axis runs over, the one named last changes fastest.
Arguments:
- ssd_x: bfloat16 [8192, 8192], P('rep', 'head'), may hold values from -6 to 6
- gate_z: bfloat16 [8192, 8192], P('rep', 'head'), may hold values from -6 to 6
- group_b: bfloat16 [8192, 1024], P('rep', 'head'), may hold values from -6 to 6
- group_c: bfloat16 [8192, 1024], P('rep', 'head'), may hold values from -0.5 to 0.5
- step_dt: bfloat16 [8192, 128], P('rep', 'head'), may hold values from 0.5 to 2
- queries: bfloat16 [8192, 8192], P('rep', 'head'), may hold values from -8 to 8
- tail_kv: bfloat16 [8192, 2048], P('rep', 'head'), may hold values from -6 to 6
- ckpt_state: bfloat16 [512, 128, 64, 128], P('rep', 'head'), may hold values from -6 to 6
- kv_pool: bfloat16 [8192, 16, 2048], P('rep', None, 'head'), may hold values from -8 to 8
- w_out: bfloat16 [8192, 4096], P('head', 'rep'), may hold values from -0.125 to 0.125
- decay_rate: float32 [128], P('head'), may hold values from 0.002 to 2
- skip_d: float32 [128], P('head'), may hold values from 0.5 to 1.5
- norm_gain: float32 [8192], P('head'), may hold values from 0.5 to 1.5
- owner: int32 [512], replicated, may hold values from 0 to 31, as said below
- slot: int32 [512], replicated, may hold values from 0 to 15, as said below
- page_table: int32 [512, 16], replicated, may hold values from 0 to 255, as said below
- hit_len: int32 [512], replicated, may hold values from 2 to 256, as said below
- tail_len: int32 [512], replicated, may hold values from 1 to 16, as said below
Outputs:
- ssd_out: bfloat16 [8192, 8192], P('rep', 'head')
- attn_proj: bfloat16 [8192, 4096], P('rep', 'head')
- final_state: bfloat16 [512, 128, 64, 128], P('rep', 'head')
The draws below stay inside these ranges and needn't reach their ends.
Inputs may be any that keep to these rules, and one draw needn't show every extreme that they name: Every replica owns exactly 16 requests, and no two requests of one replica share an owner. `slot`: the requests of one owner have distinct slots. `page_table`: each of an owner's 256 pages belongs to exactly one of its requests. `hit_len`: some request has exactly 256. `tail_len`: some request has exactly 16.
All inputs are finite; a program needn't handle non-finite values.
Results may differ from the reference program's by a relative error of at most 0.0057.
Values may be sent and summed in bfloat16 or wider, within the bound.
No kernel may reach another device: no remote copies, remote signals or barrier semaphores. Data moves between devices by JAX's collectives and lax.ppermute only.
A program may use at most 192 MiB of HBM per device.

```python
import math
import jax
import jax.numpy as jnp
from jax import lax

REQ_DEV = 16
TAIL = 16
CACHE = 256
PAGE = 16
SSD_DEV = 16
HEAD_DIM = 64
STATE = 128
QH_DEV = 8
DH = 128
D_OUT = 4096
REQS = 512
TOKENS = 8192
PAGES_REQ = 16
POOL_DEV = 256
POOL = 8192
SSD_HEADS = 128
QHEADS = 64
KV_WIDTH = 2048
N_REP = 32
N_HEAD = 8


def choose_owners(key):
    base = jax.random.fold_in(key, 11)
    first_key, second_key, third_key, fourth_key = jax.random.split(base, 4)
    replicas = REQS // REQ_DEV
    order = jax.random.permutation(first_key, replicas)
    places = jax.random.permutation(second_key, replicas)
    shifts = jax.random.permutation(third_key, replicas)[:REQ_DEV]
    owners = order[(places[:, None] + shifts[None, :]) % replicas]
    scores = jax.random.randint(fourth_key, (replicas, REQ_DEV), 0, 1 << 16) * REQ_DEV + jnp.arange(REQ_DEV)[None, :]
    ranking = jnp.argsort(scores, axis=1)
    slot_ids = ranking[owners, jnp.arange(REQ_DEV)[None, :]]
    return (owners.reshape(-1).astype(jnp.int32), slot_ids.reshape(-1).astype(jnp.int32))


def draw_owner(key, part):
    return choose_owners(key)[0]


def draw_slot(key, part):
    return choose_owners(key)[1]


def draw_page_table(key, part):
    owners, slot_ids = choose_owners(key)
    replicas = REQS // REQ_DEV
    scores = jax.random.randint(jax.random.fold_in(key, 13), (replicas, POOL_DEV), 0, 1 << 16) * POOL_DEV + jnp.arange(POOL_DEV)[None, :]
    ranking = jnp.argsort(scores, axis=1)
    columns = slot_ids[:, None] * PAGES_REQ + jnp.arange(PAGES_REQ)[None, :]
    return ranking[owners[:, None], columns].astype(jnp.int32)


def draw_hit_len(key, part):
    values = jax.random.randint(jax.random.fold_in(key, 17), (REQS,), 2, CACHE + 1)
    chosen = jax.random.randint(jax.random.fold_in(key, 19), (), 0, REQS)
    return values.at[chosen].set(CACHE).astype(jnp.int32)


def draw_tail_len(key, part):
    values = jax.random.randint(jax.random.fold_in(key, 23), (REQS,), 1, TAIL + 1)
    chosen = jax.random.randint(jax.random.fold_in(key, 29), (), 0, REQS)
    return values.at[chosen].set(TAIL).astype(jnp.int32)


def draw_queries(key, part):
    inner_key = jax.random.fold_in(key, 37)
    shape = (TOKENS, QHEADS * DH)
    values = jax.random.truncated_normal(inner_key, -8.0, 8.0, shape, jnp.float32)
    return values.astype(jnp.bfloat16)


def draw_kv_pool(key, part):
    inner_key = jax.random.fold_in(key, 41)
    shape = (POOL, PAGE, KV_WIDTH)
    values = jax.random.truncated_normal(inner_key, -8.0, 8.0, shape, jnp.float32)
    return values.astype(jnp.bfloat16)


def spiked(values, stream_key, source, target, shards_of, factor):
    owner, partner = [(jnp.arange(values.shape[dim]) // (values.shape[dim] // shards_of)).reshape([-1 if axis == dim else 1 for axis in range(values.ndim)]) for dim in (source, target)]
    chosen = jax.random.permutation(stream_key, shards_of)[partner]
    strong = (owner == chosen) | (owner == (partner + shards_of // 2) % shards_of)
    return jnp.where(strong, factor * values, values)


def levels(key, shape, cuts, least, high):
    def one(axis_at, shards_of):
        draws = jax.random.uniform(jax.random.fold_in(jax.random.fold_in(key, 6), axis_at), (shards_of,), jnp.float32, least / len(cuts), high / len(cuts))
        return jnp.repeat(jnp.exp(draws), shape[axis_at] // shards_of).reshape((-1,) + (1,) * (len(shape) - axis_at - 1))

    factor_of = one(*cuts[0])
    for cut in cuts[1:]:
        factor_of = factor_of * one(*cut)
    return factor_of


def normal_values(stream_key, shape, deviation, limit, shards=(), kind=jnp.bfloat16):
    values = jax.random.normal(stream_key, shape, jnp.float32) * deviation
    if len(shards) > 0:
        values = levels(stream_key, shape, shards, -0.22, 0.18) * values
    return jnp.clip(values, min=-limit, max=limit).astype(kind)


def bell_draw_with(own_key, extent, scale, bound, cuts, heavy, held_as=jnp.bfloat16):
    values = scale * jax.random.normal(own_key, extent, jnp.float32)
    if cuts:
        values = values * levels(own_key, extent, cuts, -0.22, 0.18)
    return jnp.clip(spiked(values, jax.random.fold_in(own_key, 3), *heavy), -bound, bound).astype(held_as)


def setup_inputs(seed: int = 0) -> dict:
    keys = jax.random.split(jax.random.key(seed), 19)
    ssd_x = normal_values(keys[0], (TOKENS, SSD_HEADS * HEAD_DIM), 1.0, 6.0, ((0, 32), (1, 8)))
    gate_z = normal_values(keys[1], (TOKENS, SSD_HEADS * HEAD_DIM), 1.0, 6.0, ((0, 32), (1, 8)))
    group_b = normal_values(keys[2], (TOKENS, STATE * N_HEAD), 1.0, 6.0, ((0, 32), (1, 8)))
    group_c = normal_values(keys[3], (TOKENS, STATE * N_HEAD), STATE ** -0.5, 0.5, ((0, 32), (1, 8)))
    step_dt = jnp.clip(jnp.exp(math.log(2.0) - 1.3862944 * jax.random.uniform(keys[4], (TOKENS, SSD_HEADS), jnp.float32) ** levels(keys[4], (TOKENS, SSD_HEADS), ((0, 32), (1, 8)), -0.2, 0.2)), 0.5, 2.0).astype(jnp.bfloat16)
    queries = draw_queries(jax.random.fold_in(keys[18], 71), 0)
    tail_kv = normal_values(keys[6], (TOKENS, KV_WIDTH), 1.0, 6.0, ((0, 32), (1, 8)))
    ckpt_state = normal_values(keys[7], (REQS, SSD_HEADS, HEAD_DIM, STATE), 1.0, 6.0, ((0, 32), (1, 8)))
    kv_pool = draw_kv_pool(jax.random.fold_in(keys[18], 71), 0)
    w_out = bell_draw_with(keys[9], (QHEADS * DH, D_OUT), (QHEADS * DH) ** -0.5, 0.125, ((0, 8), (1, 32)), (0, 1, 32, 2.75))
    decay_rate = jnp.clip(jnp.exp(math.log(2.0) - 6.9077552 * jax.random.uniform(keys[10], (SSD_HEADS,), jnp.float32) ** levels(keys[10], (SSD_HEADS,), ((0, 8),), -0.2, 0.2)), 0.002, 2.0)
    skip_d = jnp.clip(0.5 + 1.0 * jax.random.uniform(keys[11], (SSD_HEADS,), jnp.float32) ** levels(keys[11], (SSD_HEADS,), ((0, 8),), -0.2, 0.2), 0.5, 1.5)
    norm_gain = jnp.clip(1.0 + 0.1 * jax.random.normal(keys[12], (SSD_HEADS * HEAD_DIM,), jnp.float32), 0.5, 1.5)
    owner = draw_owner(jax.random.fold_in(keys[18], 71), 0)
    slot = draw_slot(jax.random.fold_in(keys[18], 71), 0)
    page_table = draw_page_table(jax.random.fold_in(keys[18], 71), 0)
    hit_len = draw_hit_len(jax.random.fold_in(keys[18], 71), 0)
    tail_len = draw_tail_len(jax.random.fold_in(keys[18], 71), 0)
    return {"ssd_x": ssd_x, "gate_z": gate_z, "group_b": group_b, "group_c": group_c, "step_dt": step_dt, "queries": queries, "tail_kv": tail_kv, "ckpt_state": ckpt_state, "kv_pool": kv_pool, "w_out": w_out, "decay_rate": decay_rate, "skip_d": skip_d, "norm_gain": norm_gain, "owner": owner, "slot": slot, "page_table": page_table, "hit_len": hit_len, "tail_len": tail_len}


highest = lax.Precision.HIGHEST

def scan_heads(signal, b_rows, c_rows, step_sizes, state_start, rates, skipping, alive):
    length = signal.shape[1]
    head_count = signal.shape[2]
    fanout = head_count // b_rows.shape[2]
    log_decay = -rates[None, None, :] * step_sizes * alive[:, :, None]
    running = jnp.cumsum(log_decay, axis=1)
    position = jnp.arange(length, dtype=jnp.int32)
    causal = (position[:, None] >= position[None, :])[None, :, :, None]
    spans = running[:, :, None, :] - running[:, None, :, :]
    decays = jnp.where(causal, jnp.exp(jnp.where(causal, spans, 0.0)), 0.0)
    intersection = jnp.einsum('ktgn,kugn->ktug', c_rows, b_rows, precision=highest)
    intersection_head = jnp.repeat(intersection, fanout, axis=3)
    weighted_dt = step_sizes * alive[:, :, None]
    mixing = decays * intersection_head * weighted_dt[:, None, :, :]
    within = jnp.einsum('ktue,kuep->ktep', mixing, signal, precision=highest)
    c_heads = jnp.repeat(c_rows, fanout, axis=2)
    b_heads = jnp.repeat(b_rows, fanout, axis=2)
    from_state = jnp.exp(running)[..., None] * jnp.einsum('kten,kepn->ktep', c_heads, state_start, precision=highest)
    mixer = (within + from_state + skipping[None, None, :, None] * signal) * alive[:, :, None, None]
    last_cum = running[:, -1, :]
    weights_in = jnp.exp(last_cum[:, None, :] - running) * weighted_dt
    closing = jnp.exp(last_cum)[:, :, None, None] * state_start + jnp.einsum('kue,kuen,kuep->kepn', weights_in, b_heads, signal, precision=highest)
    return (mixer, closing)

def attend(query_rows, cached, tail_rows, hit_sizes, tail_sizes, alive):
    batch = query_rows.shape[0]
    query_len = query_rows.shape[1]
    cache_len = cached.shape[1]
    scaling = 1.0 / math.sqrt(query_rows.shape[-1])
    cached_scores = jnp.einsum('ktaqd,kcad->ktaqc', query_rows, cached[:, :, :, 0, :], precision=highest) * scaling
    tail_scores = jnp.einsum('ktaqd,kuad->ktaqu', query_rows, tail_rows[:, :, :, 0, :], precision=highest) * scaling
    positions = jnp.arange(cache_len, dtype=jnp.int32)
    position = jnp.arange(query_len, dtype=jnp.int32)
    seen_cache = jnp.broadcast_to((positions[None, :] < hit_sizes[:, None])[:, None, :], (batch, query_len, cache_len))
    seen_tail = (position[None, None, :] <= position[None, :, None]) & (position[None, None, :] < tail_sizes[:, None, None])
    visible = jnp.concatenate([seen_cache, seen_tail], axis=2)[:, :, None, None, :]
    scores = jnp.where(visible, jnp.concatenate([cached_scores, tail_scores], axis=4), -1e+30)
    row_max = lax.optimization_barrier(jnp.max(scores, axis=4, keepdims=True))
    exponent = jnp.where(visible, jnp.exp(scores - row_max), 0.0)
    weights = (exponent / lax.optimization_barrier(jnp.sum(exponent, axis=4, keepdims=True))).astype(jnp.bfloat16).astype(jnp.float32)
    result = jnp.einsum('ktaqc,kcad->ktaqd', weights[..., :cache_len], cached[:, :, :, 1, :], precision=highest)
    result = result + jnp.einsum('ktaqu,kuad->ktaqd', weights[..., cache_len:], tail_rows[:, :, :, 1, :], precision=highest)
    return (result * alive[:, :, None, None, None]).astype(jnp.bfloat16)

def reference(ssd_x, gate_z, group_b, group_c, step_dt, queries, tail_kv, ckpt_state, kv_pool, w_out, decay_rate, skip_d, norm_gain, owner, slot, page_table, hit_len, tail_len):
    channels = SSD_HEADS * HEAD_DIM
    group_width = SSD_DEV * HEAD_DIM

    def one_home(home):
        first_row = home * REQ_DEV
        request_ids = first_row + jnp.arange(REQ_DEV, dtype=jnp.int32)
        owners = owner[request_ids]
        slot_ids = slot[request_ids]
        hit_sizes = hit_len[request_ids]
        tail_sizes = tail_len[request_ids]
        state_start = ckpt_state[owners * REQ_DEV + slot_ids].astype(jnp.float32)
        page_rows = kv_pool[owners[:, None] * POOL_DEV + page_table[request_ids]]
        cached = page_rows.reshape(REQ_DEV, CACHE, N_HEAD, 2, DH).astype(jnp.float32)

        def per_request(array):
            block = lax.dynamic_slice_in_dim(array, (first_row * TAIL).astype(jnp.int32), REQ_DEV * TAIL, 0)
            return block.reshape(REQ_DEV, TAIL, -1)
        alive = (jnp.arange(TAIL, dtype=jnp.int32)[None, :] < tail_sizes[:, None]).astype(jnp.float32)
        signal = per_request(ssd_x).reshape(REQ_DEV, TAIL, SSD_HEADS, HEAD_DIM).astype(jnp.float32)
        b_rows = per_request(group_b).reshape(REQ_DEV, TAIL, N_HEAD, STATE).astype(jnp.float32)
        c_rows = per_request(group_c).reshape(REQ_DEV, TAIL, N_HEAD, STATE).astype(jnp.float32)
        step_sizes = per_request(step_dt).astype(jnp.float32)
        mixer, closing = scan_heads(signal, b_rows, c_rows, step_sizes, state_start, decay_rate, skip_d, alive)
        gate_rows = per_request(gate_z).reshape(REQ_DEV, TAIL, SSD_HEADS, HEAD_DIM).astype(jnp.float32)
        gated_out = (mixer * jax.nn.silu(gate_rows)).reshape(REQ_DEV, TAIL, N_HEAD, group_width)
        energy = lax.optimization_barrier(jnp.sum(gated_out * gated_out, axis=3, keepdims=True))
        normed = gated_out / jnp.sqrt(energy / group_width + 1e-05) * norm_gain.reshape(N_HEAD, group_width)
        query_rows = per_request(queries).reshape(REQ_DEV, TAIL, N_HEAD, QH_DEV, DH).astype(jnp.float32)
        tail_rows = per_request(tail_kv).reshape(REQ_DEV, TAIL, N_HEAD, 2, DH).astype(jnp.float32)
        attention = attend(query_rows, cached, tail_rows, hit_sizes, tail_sizes, alive)
        projected = jnp.dot(attention.reshape(REQ_DEV * TAIL, QHEADS * DH), w_out, preferred_element_type=jnp.float32)
        return (normed.astype(jnp.bfloat16).reshape(REQ_DEV * TAIL, channels), projected.astype(jnp.bfloat16), closing.astype(jnp.bfloat16))
    gathered = lax.map(one_home, jnp.arange(N_REP, dtype=jnp.int32))
    return (gathered[0].reshape(TOKENS, SSD_HEADS * HEAD_DIM), gathered[1].reshape(TOKENS, D_OUT), gathered[2].reshape(REQS, SSD_HEADS, HEAD_DIM, STATE))
```

```python
import math

import jax
import jax.numpy as jnp
from jax import lax
from jax.experimental import pallas as pl
from jax.experimental.pallas import tpu as pltpu
from jax.sharding import PartitionSpec as P


TAIL = 16
STATE = 128
QH = 8
DH = 128
REQ = 16
REPS = 32
HEADS = 16
HD = 64
PAGES = 16
CACHE = 256
TOK = REQ * TAIL
WIDTH = HEADS * HD
QW = QH * DH + 2 * DH
NHEAD = 8
NEAR = (0, -1, 1, 2)
SIZES = (14, 2)
STARTS = (0, 14)
STEPS = (2, 4)
CHUNKS = len(SIZES)
ROOM = 4 * TAIL * DH // (HD * STATE)

f32 = jnp.float32
bf16 = jnp.bfloat16
SMEM = pl.BlockSpec(memory_space=pltpu.SMEM)
VMEM = pl.BlockSpec(memory_space=pltpu.VMEM)
ANY = pl.BlockSpec(memory_space=pl.ANY)
NT = (((1,), (1,)), ((), ()))


def dot(a, b):
    return jnp.dot(a, b, preferred_element_type=f32)


def split2(v):
    hi = v.astype(bf16)
    return hi, (v - hi.astype(f32)).astype(bf16)


def split3(v):
    hi = v.astype(bf16)
    rest = v - hi.astype(f32)
    mid = rest.astype(bf16)
    return hi, mid, (rest - mid.astype(f32)).astype(bf16)


def sds(shape, dtype):
    return jax.ShapeDtypeStruct(shape, dtype)


def params(**kw):
    return pltpu.CompilerParams(**kw)


def pack_q_body(me, owner, q, kv, out, sem):
    base = me[0] * REQ
    for j in range(REQ):
        o = owner[base + j]
        rows = pl.ds(j * TAIL, TAIL)
        pltpu.make_async_copy(q.at[rows], out.at[o, :, pl.ds(0, QH * DH)], sem.at[0]).start()
        pltpu.make_async_copy(kv.at[rows], out.at[o, :, pl.ds(QH * DH, 2 * DH)], sem.at[1]).start()
    pltpu.make_async_copy(q, q, sem.at[0]).wait()
    pltpu.make_async_copy(kv, kv, sem.at[1]).wait()


def pack_q(me, owner, q, kv):
    return pl.pallas_call(
        pack_q_body,
        out_shape=sds((REPS, TAIL, QW), bf16),
        in_specs=[SMEM, SMEM, VMEM, VMEM],
        out_specs=ANY,
        scratch_shapes=[pltpu.SemaphoreType.DMA((2,))],
        name="pack_q",
    )(me, owner, q, kv)


def pack_s_body(me, owner, slot, ckpt, *rest):
    outs = rest[:CHUNKS]
    req, buf, come, go = rest[CHUNKS:]
    mine = me[0]
    for s in range(REQ):
        pltpu.make_async_copy(ckpt.at[s], buf.at[s], come.at[s]).start()

    def home(h, carry):
        s = jnp.int32(0)
        g = jnp.int32(0)
        for j in range(REQ):
            hit = owner[h * REQ + j] == mine
            s = jnp.where(hit, slot[h * REQ + j] + 1, s)
            g = jnp.where(hit, h * REQ + j, g)

        @pl.when(s > 0)
        def _():
            req[s - 1] = g

        return carry

    lax.fori_loop(0, REPS, home, 0)
    for s in range(REQ):
        pltpu.make_async_copy(ckpt.at[s], buf.at[s], come.at[s]).wait()
        for c in range(CHUNKS):
            pltpu.make_async_copy(
                buf.at[s, pl.ds(STARTS[c], SIZES[c])],
                outs[c].at[req[s] // REQ, pl.ds(0, SIZES[c])],
                go.at[c],
            ).start()
    for c in range(CHUNKS):
        part = buf.at[:, pl.ds(STARTS[c], SIZES[c])]
        pltpu.make_async_copy(part, part, go.at[c]).wait()


def pack_s(me, owner, slot, ckpt):
    depth = [n + (ROOM if c == CHUNKS - 1 else 0) for c, n in enumerate(SIZES)]
    out = pl.pallas_call(
        pack_s_body,
        out_shape=[sds((REPS, n, HD, STATE), bf16) for n in depth] + [sds((REQ,), jnp.int32)],
        in_specs=[SMEM, SMEM, SMEM, ANY],
        out_specs=[ANY] * CHUNKS + [SMEM],
        scratch_shapes=[
            pltpu.VMEM((REQ, HEADS, HD, STATE), bf16),
            pltpu.SemaphoreType.DMA((REQ,)),
            pltpu.SemaphoreType.DMA((CHUNKS,)),
        ],
        name="pack_s",
    )(me, owner, slot, ckpt)
    return out[:CHUNKS], out[CHUNKS]


def attend_body(req, pages, hit, tail, qin, pool, out):
    row = lax.broadcasted_iota(jnp.int32, (QH * TAIL, CACHE + DH), 0) & (TAIL - 1)
    col = lax.broadcasted_iota(jnp.int32, (QH * TAIL, CACHE + DH), 1)
    late = col - CACHE
    causal = (late >= 0) & (late <= row)
    time = lax.broadcasted_iota(jnp.int32, (QH * TAIL, DH), 0) & (TAIL - 1)
    pad = jnp.zeros((DH - TAIL, DH), bf16)
    scale = 1.0 / math.sqrt(DH)

    def one(s, carry):
        g = req[s]
        q = qin[g // REQ]
        rows = jnp.concatenate([q[:, a * DH : (a + 1) * DH] for a in range(QH)], axis=0)
        held = [pool[pages[g * PAGES + i]] for i in range(PAGES)]
        keys = jnp.concatenate(
            [p[:, :DH] for p in held] + [q[:, QH * DH : QH * DH + DH], pad], axis=0
        )
        vals = jnp.concatenate([p[:, DH:] for p in held] + [q[:, QH * DH + DH :], pad], axis=0)
        scores = lax.dot_general(rows, keys, NT, preferred_element_type=f32) * scale
        visible = (col < hit[g]) | (causal & (late < tail[g]))
        scores = jnp.where(visible, scores, -1e30)
        top = jnp.max(scores, axis=1, keepdims=True)
        expo = jnp.where(visible, jnp.exp(scores - top), 0.0)
        weights = (expo / jnp.sum(expo, axis=1, keepdims=True)).astype(bf16)
        res = dot(weights, vals)
        res = jnp.where(time < tail[g], res, 0.0).astype(bf16)
        for a in range(QH):
            out[pl.ds(pl.multiple_of(s * TAIL, TAIL), TAIL), a * DH : (a + 1) * DH] = res[
                a * TAIL : (a + 1) * TAIL
            ]
        return carry

    lax.fori_loop(0, REQ, one, 0, unroll=2)


def attend(req, pages, hit, tail, qin, pool):
    return pl.pallas_call(
        attend_body,
        out_shape=sds((TOK, QH * DH), bf16),
        in_specs=[SMEM, SMEM, SMEM, SMEM, VMEM, VMEM],
        out_specs=VMEM,
        cost_estimate=pl.CostEstimate(
            flops=8_000_000_000, transcendentals=0, bytes_accessed=4_000_000
        ),
        name="attend",
    )(req, pages, hit, tail, qin, pool)


def spot(k, i):
    base = jnp.int32(12)
    for dist, start in ((1, 16), (2, 0), (3, 20), (5, 28), (6, 6), (7, 24)):
        base = jnp.where(k == dist, start, base)
    base = jnp.where(k == 4, jnp.where(i < 2, 4, 8), base)
    return base + i


def project_body(me, head, attn, a_near, b_near, a_far, b_far, out):
    x = me[0] // 8
    y = (me[0] // 2) & 3
    par = me[0] & 1
    step = pl.program_id(0)
    off = jnp.where(step == 3, 2, jnp.where(step == 1, -1, jnp.where(step == 2, 1, 0)))
    cy = (y + off) & 3
    half = QH * DH // 2
    for far, (wa, wb) in enumerate(((a_near, b_near), (a_far, b_far))):
        core = 1 - par if far else par
        for d in (0, 2):
            res = dot(attn[:, :half], jnp.concatenate([wa[0, d], wa[0, d + 1]], axis=1)) + dot(
                attn[:, half:], jnp.concatenate([wb[d, 0], wb[d + 1, 0]], axis=1)
            )
            res = res.astype(bf16)
            for k in range(2):
                col = ((x + NEAR[d + k]) & 3) * 8 + cy * 2 + core
                out[spot(((col // 4) - head[0]) & (NHEAD - 1), col & 3)] = res[
                    :, k * DH : (k + 1) * DH
                ]


def project(me, head, attn, a_near, b_near, a_far, b_far):
    half = QH * DH // 2
    wa = pl.BlockSpec((1, 4, half, DH), lambda i: (i, 0, 0, 0))
    wb = pl.BlockSpec((4, 1, half, DH), lambda i: (0, i, 0, 0))
    return pl.pallas_call(
        project_body,
        grid=(4,),
        out_shape=sds((4 * NHEAD, TOK, DH), bf16),
        in_specs=[SMEM, SMEM, pl.BlockSpec((TOK, QH * DH), lambda i: (0, 0)), wa, wb, wa, wb],
        out_specs=pl.BlockSpec((4 * NHEAD, TOK, DH), lambda i: (0, 0, 0)),
        compiler_params=params(dimension_semantics=("arbitrary",)),
        cost_estimate=pl.CostEstimate(
            flops=8_000_000_000, transcendentals=0, bytes_accessed=11_000_000
        ),
        name="project",
    )(me, head, attn, a_near, b_near, a_far, b_far)


def relay_body(terms, up, down, one, three, seven, five):
    def add(a, b):
        return (a.astype(f32) + b.astype(f32)).astype(bf16)

    one[...] = add(terms[16:20], up[0:4])
    three[0:2] = add(terms[20:22], up[4:6])
    three[2:4] = terms[22:24]
    seven[...] = add(terms[24:28], down[0:4])
    five[0:2] = terms[28:30]
    five[2:4] = add(terms[30:32], down[4:6])


def relay(terms, up, down):
    return pl.pallas_call(
        relay_body,
        out_shape=[sds((4, TOK, DH), bf16)] * 4,
        in_specs=[VMEM] * 3,
        out_specs=[VMEM] * 4,
        cost_estimate=pl.CostEstimate(
            flops=1_000_000_000, transcendentals=0, bytes_accessed=3_000_000
        ),
        name="relay",
    )(terms, up, down)


def total_body(req, terms, *rest):
    parts = rest[:4]
    out, tmp, sem = rest[5:]
    for i in range(4):
        acc = terms[12 + i].astype(f32)
        for p in parts:
            acc = acc + p[i].astype(f32)
        acc = acc.astype(bf16)
        for s in range(REQ):
            tmp[s, i * TAIL : (i + 1) * TAIL, :] = acc[s * TAIL : (s + 1) * TAIL]
    for s in range(REQ):
        pltpu.make_async_copy(tmp.at[s], out.at[req[s] // REQ, SIZES[-1]], sem.at[0]).start()
    pltpu.make_async_copy(tmp, tmp, sem.at[0]).wait()


def total(req, terms, parts, packed):
    return pl.pallas_call(
        total_body,
        out_shape=sds(packed.shape, bf16),
        in_specs=[SMEM] + [VMEM] * 5 + [ANY],
        out_specs=ANY,
        input_output_aliases={6: 0},
        scratch_shapes=[pltpu.VMEM((REQ, 4 * TAIL, DH), bf16), pltpu.SemaphoreType.DMA((1,))],
        cost_estimate=pl.CostEstimate(
            flops=1_000_000_000, transcendentals=0, bytes_accessed=3_000_000
        ),
        name="total",
    )(req, terms, *parts, packed)


def prepare_body(
    me, tail, x_ref, z_ref, b_ref, c_ref, dt_ref, rate, skip, base_ref, ecx_ref, xt_ref, dl_ref, tmp
):
    first = me[0] * REQ
    req16 = lax.broadcasted_iota(jnp.int32, (TOK, HEADS), 0) // TAIL
    tim16 = lax.broadcasted_iota(jnp.int32, (TOK, HEADS), 0) & (TAIL - 1)
    limit = jnp.zeros((TOK, HEADS), jnp.int32)
    for j in range(REQ):
        limit = jnp.where(req16 == j, tail[first + j], limit)
    live = (tim16 < limit).astype(f32)
    wdt = dt_ref[...].astype(f32) * live
    decay = -rate[...] * wdt
    r = lax.broadcasted_iota(jnp.int32, (TOK, TOK), 0)
    u = lax.broadcasted_iota(jnp.int32, (TOK, TOK), 1)
    same = (r // TAIL) == (u // TAIL)
    tri = same & (u <= r)
    trib = tri.astype(f32).astype(bf16)
    allb = same.astype(f32).astype(bf16)
    pieces = split3(decay)
    cum = dot(trib, pieces[0]) + dot(trib, pieces[1]) + dot(trib, pieces[2])
    last = dot(allb, pieces[0]) + dot(allb, pieces[1]) + dot(allb, pieces[2])
    tmp[...] = jnp.exp(last)
    dl_ref[...] = tmp[pl.ds(0, REQ, stride=TAIL), :]
    er = lax.broadcasted_iota(jnp.int32, (HEADS, WIDTH), 0)
    ec = lax.broadcasted_iota(jnp.int32, (HEADS, WIDTH), 1)
    onehot = ((ec // HD) == er).astype(f32).astype(bf16)

    def widen(v):
        a, b, c = split3(v)
        return dot(a, onehot) + dot(b, onehot) + dot(c, onehot)

    x = x_ref[...].astype(f32)
    hi, lo = split2(widen(jnp.exp(-cum) * wdt) * x)
    cb = jnp.where(
        tri, lax.dot_general(c_ref[...], b_ref[...], NT, preferred_element_type=f32), 0.0
    )
    chi, clo = split2(cb)
    within = dot(chi, hi) + dot(chi, lo) + dot(clo, hi)
    z = z_ref[...].astype(f32)
    gate = z / (1.0 + jnp.exp(-z))
    ecx = widen(jnp.exp(cum) * live)
    base_ref[...] = (ecx * within + widen(skip[...] * live) * x) * gate
    ecx_ref[...] = ecx * gate
    hi, lo = split2(widen(jnp.exp(last - cum) * wdt) * x)
    for k in range(2):
        rows = slice(k * 128, (k + 1) * 128)
        xt_ref[k, :, :128] = hi[rows].T
        xt_ref[k, :, 128:] = lo[rows].T


def prepare(me, tail, x, z, b, c, dt, rate, skip):
    return pl.pallas_call(
        prepare_body,
        out_shape=[
            sds((TOK, WIDTH), f32),
            sds((TOK, WIDTH), f32),
            sds((2, WIDTH, 256), bf16),
            sds((REQ, HEADS), f32),
        ],
        in_specs=[SMEM, SMEM] + [VMEM] * 7,
        out_specs=[VMEM] * 4,
        scratch_shapes=[pltpu.VMEM((TOK, HEADS), f32)],
        cost_estimate=pl.CostEstimate(
            flops=8_000_000_000, transcendentals=0, bytes_accessed=5_000_000
        ),
        name="prepare",
    )(me, tail, x, z, b, c, dt, rate, skip)


def scan_body(chunk, *refs):
    refs = list(refs)
    heads = SIZES[chunk]
    count = STEPS[chunk]
    width = heads * HD
    final_chunk = chunk == CHUNKS - 1
    dl = refs[2]
    held = refs[3 : 3 + count]
    b_ref, c_ref, xt, base, ecx = refs[3 + count : 8 + count]
    refs = refs[8 + count :]
    prev = []
    if chunk > 0:
        prev = refs[1 : 1 + chunk]
        refs = refs[1 + chunk :]
    if final_chunk:
        gain, fin, out, proj = refs
    else:
        fin, gated_ref = refs
    i = pl.program_id(0)
    states = [s[0, :heads].reshape(width, STATE) for s in held]
    seen = jnp.concatenate(
        [
            lax.dot_general(
                c_ref[k * TAIL : (k + 1) * TAIL, :], states[k], NT, preferred_element_type=f32
            )
            for k in range(count)
        ],
        axis=0,
    )
    gated = base[...] + ecx[...] * seen
    if final_chunk:
        parts = [p[...] for p in prev] + [gated]
        energy = sum(jnp.sum(p * p, axis=1, keepdims=True) for p in parts)
        denom = jnp.sqrt(energy / WIDTH + 1e-5)
        for c in range(CHUNKS):
            cols = slice(STARTS[c] * HD, (STARTS[c] + SIZES[c]) * HD)
            out[:, cols] = (parts[c] / denom * gain[:, cols]).astype(bf16)
        for k, s in enumerate(held):
            for c in range(4):
                proj[k * TAIL : (k + 1) * TAIL, c * DH : (c + 1) * DH] = s[
                    0, heads, c * TAIL : (c + 1) * TAIL, :
                ]
    else:
        gated_ref[...] = gated
    who = lax.broadcasted_iota(jnp.int32, (128, STATE), 0) // TAIL
    rows = b_ref[...].astype(f32)
    at = (count * i) & 7
    mine = jnp.concatenate(
        [jnp.where(who == at + k, rows, 0.0).astype(bf16) for k in range(count)], axis=1
    )
    update = dot(xt[0], jnp.concatenate([mine, mine], axis=0))
    for k in range(count):
        for e in range(heads):
            rr = slice(e * HD, (e + 1) * HD)
            fin[k, e] = (
                dl[count * i + k, STARTS[chunk] + e] * states[k][rr].astype(f32)
                + update[rr, k * STATE : (k + 1) * STATE]
            ).astype(bf16)


def scan(chunk, me, owner, dl, got, b, c, xt, base, ecx, fin, prev, gain):
    final_chunk = chunk == CHUNKS - 1
    heads = SIZES[chunk]
    count = STEPS[chunk]
    width = heads * HD
    at = STARTS[chunk] // heads
    rows = count * TAIL

    def held(k):
        return pl.BlockSpec(
            (1,) + got.shape[1:], lambda i, m, o: (o[m[0] * REQ + count * i + k], 0, 0, 0)
        )

    def span(w, col=0):
        return pl.BlockSpec((rows, w), lambda i, m, o: (i, col))

    in_specs = [SMEM] + [held(k) for k in range(count)]
    in_specs += [
        pl.BlockSpec((128, STATE), lambda i, m, o: (i * count // 8, 0)),
        span(STATE),
        pl.BlockSpec((1, width, 256), lambda i, m, o: (i * count // 8, at, 0)),
        span(width, at),
        span(width, at),
    ]
    args = [dl] + [got] * count + [b, c, xt, base, ecx]
    alias = {}
    if chunk > 0:
        alias = {2 + len(args): 0}
        in_specs += [ANY] + [span(p.shape[1]) for p in prev]
        args += [fin] + prev
    out_specs = [pl.BlockSpec((count, heads, HD, STATE), lambda i, m, o: (i, at, 0, 0))]
    out_shape = [sds((REQ, HEADS, HD, STATE), bf16)]
    if final_chunk:
        in_specs.append(pl.BlockSpec((1, WIDTH), lambda i, m, o: (0, 0)))
        args.append(gain)
        out_specs += [span(WIDTH), span(4 * DH)]
        out_shape += [sds((TOK, WIDTH), bf16), sds((TOK, 4 * DH), bf16)]
    else:
        out_specs += [span(width)]
        out_shape += [sds((TOK, width), f32)]

    def body(*refs):
        scan_body(chunk, *refs)

    return pl.pallas_call(
        body,
        grid_spec=pltpu.PrefetchScalarGridSpec(
            num_scalar_prefetch=2,
            grid=(REQ // count,),
            in_specs=in_specs,
            out_specs=out_specs,
        ),
        out_shape=out_shape,
        input_output_aliases=alias,
        compiler_params=params(dimension_semantics=("arbitrary",)),
        cost_estimate=pl.CostEstimate(
            flops=4_000_000_000, transcendentals=0, bytes_accessed=8_000_000
        ),
    )(me, owner, *args)


def exchange(x, axis):
    return lax.all_to_all(x, axis, split_axis=0, concat_axis=0, tiled=True)


def place(x, y, core):
    return (x & 3) * 8 + (y & 3) * 2 + core


def hop(v, axis, by):
    dx, dy = (by, 0) if axis == "x" else (0, by)
    pairs = [
        (place(x, y, c), place(x + dx, y + dy, c))
        for x in range(4)
        for y in range(4)
        for c in range(2)
    ]
    return lax.ppermute(v, "rep", pairs)


def ring(v, axis):
    return jnp.stack([v, hop(v, axis, 1), hop(v, axis, -1), hop(v, axis, 2)])


def sides(v, axis):
    return hop(v, axis, 1), hop(v, axis, -1)


def across(v, axis, left, right):
    n = v.shape[0] // 2
    far = jnp.concatenate([hop(right[:n], axis, -1), hop(left[n:], axis, 1)], axis=0)
    return jnp.stack([v, left, right, far])


def turn(v, by):
    return lax.ppermute(v, "head", [(z, (z + by) % NHEAD) for z in range(NHEAD)])


def step(
    ssd_x,
    gate_z,
    group_b,
    group_c,
    step_dt,
    queries,
    tail_kv,
    ckpt_state,
    kv_pool,
    w_out,
    decay_rate,
    skip_d,
    norm_gain,
    owner,
    slot,
    page_table,
    hit_len,
    tail_len,
):
    me = lax.axis_index("rep").astype(jnp.int32).reshape(1)
    head = lax.axis_index("head").astype(jnp.int32).reshape(1)
    swap = [(r, r ^ 1) for r in range(REPS)]
    half = w_out.shape[0] // 2
    queued = pack_q(me, owner, queries, tail_kv)
    asked = exchange(queued, "rep")
    w_out = lax.optimization_barrier((w_out, queued))[0]
    a_half = ring(w_out[:half], "x")
    b_half = ring(w_out[half:], "y")
    a_side = sides(a_half, "y")
    b_side = sides(b_half, "x")
    a_near = across(a_half, "y", *a_side)
    b_near = across(b_half, "x", *b_side)
    a_far = lax.ppermute(a_near, "rep", swap)
    b_far = lax.ppermute(b_near, "rep", swap)
    packed, req = pack_s(me, owner, slot, ckpt_state)
    first = lax.optimization_barrier((packed[0], asked, a_near, b_near))[0]
    got = exchange(first, "rep")
    attn = attend(req, page_table.reshape(-1), hit_len, tail_len, asked, kv_pool)
    terms = project(me, head, attn, a_near, b_near, a_far, b_far)
    one, three, seven, five = relay(terms, turn(terms[0:6], 1), turn(terms[6:12], -1))
    parts = [turn(one, 1), turn(three, 3), turn(seven, -1), turn(five, -3)]
    base, ecx, xt, dl = prepare(
        me,
        tail_len,
        ssd_x,
        gate_z,
        group_b,
        group_c,
        step_dt,
        decay_rate.reshape(1, -1),
        skip_d.reshape(1, -1),
    )
    gain = norm_gain.reshape(1, -1)
    last = exchange(total(req, terms, parts, packed[1]), "rep")
    fin, rows = scan(0, me, owner, dl, got, group_b, group_c, xt, base, ecx, None, [], gain)
    fin, out, projected = scan(
        1, me, owner, dl, last, group_b, group_c, xt, base, ecx, fin, [rows], gain
    )
    return out, projected, fin


def solution(mesh):
    return jax.shard_map(
        step,
        mesh=mesh,
        in_specs=(
            P("rep", "head"),
            P("rep", "head"),
            P("rep", "head"),
            P("rep", "head"),
            P("rep", "head"),
            P("rep", "head"),
            P("rep", "head"),
            P("rep", "head", None, None),
            P("rep", None, "head"),
            P("head", "rep"),
            P("head"),
            P("head"),
            P("head"),
            P(),
            P(),
            P(),
            P(),
            P(),
        ),
        out_specs=(P("rep", "head"), P("rep", "head"), P("rep", "head", None, None)),
        check_vma=False,
    )
```

```python
import math

import jax
import jax.numpy as jnp
from jax import lax
from jax.experimental import pallas as pl
from jax.experimental.pallas import tpu as pltpu
from jax.sharding import PartitionSpec as P


TAIL = 16
STATE = 128
QH = 8
DH = 128
REQ = 16
REPS = 32
HEADS = 16
HD = 64
PAGES = 16
CACHE = 256
TOK = REQ * TAIL
WIDTH = HEADS * HD
NHEAD = 8
NEAR = (0, -1, 1, 2)
SIZES = (14, 2)
STARTS = (0, 14)
STEPS = (2, 4)
CHUNKS = len(SIZES)
EARLY = 2 * HD
MOST = 12 * HD
LAST = 2 * HD
SLAB = 4 * TAIL
ASK = (QH + 2) * TAIL

f32 = jnp.float32
bf16 = jnp.bfloat16
SMEM = pl.BlockSpec(memory_space=pltpu.SMEM)
VMEM = pl.BlockSpec(memory_space=pltpu.VMEM)
ANY = pl.BlockSpec(memory_space=pl.ANY)
NT = (((1,), (1,)), ((), ()))


def dot(a, b):
    return jnp.dot(a, b, preferred_element_type=f32)


def split2(v):
    hi = v.astype(bf16)
    return hi, (v - hi.astype(f32)).astype(bf16)


def split3(v):
    hi = v.astype(bf16)
    rest = v - hi.astype(f32)
    mid = rest.astype(bf16)
    return hi, mid, (rest - mid.astype(f32)).astype(bf16)


def sds(shape, dtype):
    return jax.ShapeDtypeStruct(shape, dtype)


def params(**kw):
    return pltpu.CompilerParams(**kw)


def serve(owner, slot, mine, req, base):
    def home(h, carry):
        s = jnp.int32(0)
        g = jnp.int32(0)
        for j in range(REQ):
            hit = owner[h * REQ + j] == mine
            s = jnp.where(hit, slot[h * REQ + j] + 1, s)
            g = jnp.where(hit, h * REQ + j, g)

        @pl.when(s > 0)
        def _():
            req[base + s - 1] = g

        return carry

    lax.fori_loop(0, REPS, home, 0)


def pack_first_body(me, owner, slot, q, kv, ckpt, out, req, buf, tmp, come, go):
    for s in range(REQ):
        pltpu.make_async_copy(ckpt.at[s, pl.ds(MOST, EARLY)], buf.at[s], come.at[s]).start()
    first = me[0] * REQ
    for j in range(REQ):
        rows = slice(j * TAIL, (j + 1) * TAIL)
        for a in range(QH):
            tmp[j, a * TAIL : (a + 1) * TAIL, :] = q[rows, a * DH : (a + 1) * DH]
        for a in range(2):
            tmp[j, (QH + a) * TAIL : (QH + a + 1) * TAIL, :] = kv[rows, a * DH : (a + 1) * DH]
        pltpu.make_async_copy(
            tmp.at[j], out.at[owner[first + j], pl.ds(EARLY, ASK)], go.at[0]
        ).start()
    serve(owner, slot, me[0], req, 0)
    for s in range(REQ):
        pltpu.make_async_copy(ckpt.at[s, pl.ds(MOST, EARLY)], buf.at[s], come.at[s]).wait()
        pltpu.make_async_copy(buf.at[s], out.at[req[s] // REQ, pl.ds(0, EARLY)], go.at[1]).start()
    pltpu.make_async_copy(tmp, tmp, go.at[0]).wait()
    pltpu.make_async_copy(buf, buf, go.at[1]).wait()


def pack_first(me, owner, slot, q, kv, ckpt):
    return pl.pallas_call(
        pack_first_body,
        out_shape=[sds((REPS, EARLY + ASK, STATE), bf16), sds((REQ,), jnp.int32)],
        in_specs=[SMEM, SMEM, SMEM, VMEM, VMEM, ANY],
        out_specs=[ANY, SMEM],
        scratch_shapes=[
            pltpu.VMEM((REQ, EARLY, STATE), bf16),
            pltpu.VMEM((REQ, ASK, DH), bf16),
            pltpu.SemaphoreType.DMA((REQ,)),
            pltpu.SemaphoreType.DMA((2,)),
        ],
        name="pack_first",
    )(me, owner, slot, q, kv, ckpt)


def pack_s_body(me, owner, slot, req, ckpt, most, last, both, buf, come, go):
    for s in range(REQ):
        pltpu.make_async_copy(ckpt.at[s], buf.at[s], come.at[s]).start()
    for s in range(REQ):
        pltpu.make_async_copy(ckpt.at[s], buf.at[s], come.at[s]).wait()
        home = req[s] // REQ
        pltpu.make_async_copy(buf.at[s, pl.ds(0, MOST)], most.at[home], go.at[0]).start()
        pltpu.make_async_copy(
            buf.at[s, pl.ds(MOST + EARLY, LAST)], last.at[home, pl.ds(0, LAST)], go.at[1]
        ).start()
    par = me[0] & 1
    for s in range(REQ):
        both[par * REQ + s] = req[s]
    serve(owner, slot, me[0] + 1 - 2 * par, both, (1 - par) * REQ)
    for k, part in enumerate((buf.at[:, pl.ds(0, MOST)], buf.at[:, pl.ds(MOST + EARLY, LAST)])):
        pltpu.make_async_copy(part, part, go.at[k]).wait()


def pack_s(me, owner, slot, req, ckpt):
    return pl.pallas_call(
        pack_s_body,
        out_shape=[
            sds((REPS, MOST, STATE), bf16),
            sds((REPS, LAST + SLAB, STATE), bf16),
            sds((2 * REQ,), jnp.int32),
        ],
        in_specs=[SMEM, SMEM, SMEM, SMEM, ANY],
        out_specs=[ANY, ANY, SMEM],
        scratch_shapes=[
            pltpu.VMEM((REQ, WIDTH, STATE), bf16),
            pltpu.SemaphoreType.DMA((REQ,)),
            pltpu.SemaphoreType.DMA((2,)),
        ],
        name="pack_s",
    )(me, owner, slot, req, ckpt)


def attend_body(req, pages, hit, tail, qin, pool, out):
    row = lax.broadcasted_iota(jnp.int32, (QH * TAIL, CACHE + DH), 0) & (TAIL - 1)
    col = lax.broadcasted_iota(jnp.int32, (QH * TAIL, CACHE + DH), 1)
    late = col - CACHE
    causal = (late >= 0) & (late <= row)
    time = lax.broadcasted_iota(jnp.int32, (QH * TAIL, DH), 0) & (TAIL - 1)
    pad = jnp.zeros((DH - TAIL, DH), bf16)
    scale = 1.0 / math.sqrt(DH)

    def one(s, carry):
        g = req[s]
        ask = qin[g // REQ]
        rows = ask[EARLY : EARLY + QH * TAIL]
        held = [pool[pages[g * PAGES + i]] for i in range(PAGES)]
        keys = jnp.concatenate(
            [p[:, :DH] for p in held] + [ask[EARLY + ASK - 2 * TAIL : EARLY + ASK - TAIL], pad], axis=0
        )
        vals = jnp.concatenate([p[:, DH:] for p in held] + [ask[EARLY + ASK - TAIL :], pad], axis=0)
        scores = lax.dot_general(rows, keys, NT, preferred_element_type=f32) * scale
        visible = (col < hit[g]) | (causal & (late < tail[g]))
        scores = jnp.where(visible, scores, -1e30)
        top = jnp.max(scores, axis=1, keepdims=True)
        expo = jnp.where(visible, jnp.exp(scores - top), 0.0)
        weights = (expo / jnp.sum(expo, axis=1, keepdims=True)).astype(bf16)
        res = dot(weights, vals)
        res = jnp.where(time < tail[g], res, 0.0).astype(bf16)
        for a in range(QH):
            out[pl.ds(pl.multiple_of(s * TAIL, TAIL), TAIL), a * DH : (a + 1) * DH] = res[
                a * TAIL : (a + 1) * TAIL
            ]
        return carry

    lax.fori_loop(0, REQ, one, 0, unroll=2)


def attend(req, pages, hit, tail, qin, pool):
    return pl.pallas_call(
        attend_body,
        out_shape=sds((TOK, QH * DH), bf16),
        in_specs=[SMEM, SMEM, SMEM, SMEM, VMEM, VMEM],
        out_specs=VMEM,
        cost_estimate=pl.CostEstimate(
            flops=8_000_000_000, transcendentals=0, bytes_accessed=4_000_000
        ),
        name="attend",
    )(req, pages, hit, tail, qin, pool)


def spot(k, i):
    base = jnp.int32(12)
    for dist, start in ((1, 16), (2, 0), (3, 20), (5, 28), (6, 6), (7, 24)):
        base = jnp.where(k == dist, start, base)
    base = jnp.where(k == 4, jnp.where(i < 2, 4, 8), base)
    return base + i


def project_body(me, head, mine, other, *rest):
    a_ring, b_ring, out = rest[:5], rest[5:10], rest[10]
    x = me[0] // 8
    y = (me[0] // 2) & 3
    par = me[0] & 1
    half = QH * DH // 2

    def block(ring, outer, inner):
        if outer < 3:
            return ring[outer][inner]
        return ring[3 + inner // 2][inner % 2]

    for dy in range(4):
        for dx in (0, 2):
            top = jnp.concatenate([block(a_ring, dy, dx), block(a_ring, dy, dx + 1)], axis=1)
            low = jnp.concatenate([block(b_ring, dx, dy), block(b_ring, dx + 1, dy)], axis=1)
            for attn, core in ((mine, par), (other, 1 - par)):
                res = (dot(attn[:, :half], top) + dot(attn[:, half:], low)).astype(bf16)
                for k in range(2):
                    pair = ((x + NEAR[dx + k]) & 3) * 4 + ((y + NEAR[dy]) & 3)
                    dist = ((pair // 2) - head[0]) & (NHEAD - 1)
                    out[spot(dist, 2 * (pair & 1) + core)] = res[:, k * DH : (k + 1) * DH]


def project(me, head, mine, other, a_ring, b_ring):
    return pl.pallas_call(
        project_body,
        out_shape=sds((4 * NHEAD, TOK, DH), bf16),
        in_specs=[SMEM, SMEM] + [VMEM] * 12,
        out_specs=VMEM,
        cost_estimate=pl.CostEstimate(
            flops=8_000_000_000, transcendentals=0, bytes_accessed=11_000_000
        ),
        name="project",
    )(me, head, mine, other, *a_ring, *b_ring)


def relay_body(terms, up, down, one, three, seven, five):
    def add(a, b):
        return (a.astype(f32) + b.astype(f32)).astype(bf16)

    one[...] = add(terms[16:20], up[0:4])
    three[0:2] = add(terms[20:22], up[4:6])
    three[2:4] = terms[22:24]
    seven[...] = add(terms[24:28], down[0:4])
    five[0:2] = terms[28:30]
    five[2:4] = add(terms[30:32], down[4:6])


def relay(terms, up, down):
    return pl.pallas_call(
        relay_body,
        out_shape=[sds((4, TOK, DH), bf16)] * 4,
        in_specs=[VMEM] * 3,
        out_specs=[VMEM] * 4,
        cost_estimate=pl.CostEstimate(
            flops=1_000_000_000, transcendentals=0, bytes_accessed=3_000_000
        ),
        name="relay",
    )(terms, up, down)


def total_body(both, terms, *rest):
    parts = rest[:4]
    out, tmp, sem = rest[5:]
    for u in range(4):
        acc = terms[12 + u].astype(f32)
        for p in parts:
            acc = acc + p[u].astype(f32)
        acc = acc.astype(bf16)
        i, core = u // 2, u % 2
        for s in range(REQ):
            tmp[core * REQ + s, i * TAIL : (i + 1) * TAIL, :] = acc[s * TAIL : (s + 1) * TAIL]
    for s in range(2 * REQ):
        at = LAST + (s // REQ) * 2 * TAIL
        pltpu.make_async_copy(
            tmp.at[s], out.at[both[s] // REQ, pl.ds(at, 2 * TAIL)], sem.at[0]
        ).start()
    pltpu.make_async_copy(tmp, tmp, sem.at[0]).wait()


def total(both, terms, parts, packed):
    return pl.pallas_call(
        total_body,
        out_shape=sds(packed.shape, bf16),
        in_specs=[SMEM] + [VMEM] * 5 + [ANY],
        out_specs=ANY,
        input_output_aliases={6: 0},
        scratch_shapes=[pltpu.VMEM((2 * REQ, 2 * TAIL, DH), bf16), pltpu.SemaphoreType.DMA((1,))],
        cost_estimate=pl.CostEstimate(
            flops=1_000_000_000, transcendentals=0, bytes_accessed=3_000_000
        ),
        name="total",
    )(both, terms, *parts, packed)


def prepare_body(
    me, tail, x_ref, z_ref, b_ref, c_ref, dt_ref, rate, skip, base_ref, ecx_ref, xt_ref, dl_ref, tmp
):
    first = me[0] * REQ
    req16 = lax.broadcasted_iota(jnp.int32, (TOK, HEADS), 0) // TAIL
    tim16 = lax.broadcasted_iota(jnp.int32, (TOK, HEADS), 0) & (TAIL - 1)
    limit = jnp.zeros((TOK, HEADS), jnp.int32)
    for j in range(REQ):
        limit = jnp.where(req16 == j, tail[first + j], limit)
    live = (tim16 < limit).astype(f32)
    wdt = dt_ref[...].astype(f32) * live
    decay = -rate[...] * wdt
    r = lax.broadcasted_iota(jnp.int32, (TOK, TOK), 0)
    u = lax.broadcasted_iota(jnp.int32, (TOK, TOK), 1)
    same = (r // TAIL) == (u // TAIL)
    tri = same & (u <= r)
    trib = tri.astype(f32).astype(bf16)
    allb = same.astype(f32).astype(bf16)
    pieces = split3(decay)
    cum = dot(trib, pieces[0]) + dot(trib, pieces[1]) + dot(trib, pieces[2])
    last = dot(allb, pieces[0]) + dot(allb, pieces[1]) + dot(allb, pieces[2])
    tmp[...] = jnp.exp(last)
    dl_ref[...] = tmp[pl.ds(0, REQ, stride=TAIL), :]
    er = lax.broadcasted_iota(jnp.int32, (HEADS, WIDTH), 0)
    ec = lax.broadcasted_iota(jnp.int32, (HEADS, WIDTH), 1)
    onehot = ((ec // HD) == er).astype(f32).astype(bf16)

    def widen(v):
        a, b, c = split3(v)
        return dot(a, onehot) + dot(b, onehot) + dot(c, onehot)

    x = x_ref[...].astype(f32)
    hi, lo = split2(widen(jnp.exp(-cum) * wdt) * x)
    cb = jnp.where(
        tri, lax.dot_general(c_ref[...], b_ref[...], NT, preferred_element_type=f32), 0.0
    )
    chi, clo = split2(cb)
    within = dot(chi, hi) + dot(chi, lo) + dot(clo, hi)
    z = z_ref[...].astype(f32)
    gate = z / (1.0 + jnp.exp(-z))
    ecx = widen(jnp.exp(cum) * live)
    base_ref[...] = (ecx * within + widen(skip[...] * live) * x) * gate
    ecx_ref[...] = ecx * gate
    hi, lo = split2(widen(jnp.exp(last - cum) * wdt) * x)
    for k in range(2):
        rows = slice(k * 128, (k + 1) * 128)
        xt_ref[k, :, :128] = hi[rows].T
        xt_ref[k, :, 128:] = lo[rows].T


def prepare(me, tail, x, z, b, c, dt, rate, skip):
    return pl.pallas_call(
        prepare_body,
        out_shape=[
            sds((TOK, WIDTH), f32),
            sds((TOK, WIDTH), f32),
            sds((2, WIDTH, 256), bf16),
            sds((REQ, HEADS), f32),
        ],
        in_specs=[SMEM, SMEM] + [VMEM] * 7,
        out_specs=[VMEM] * 4,
        scratch_shapes=[pltpu.VMEM((TOK, HEADS), f32)],
        cost_estimate=pl.CostEstimate(
            flops=8_000_000_000, transcendentals=0, bytes_accessed=5_000_000
        ),
        name="prepare",
    )(me, tail, x, z, b, c, dt, rate, skip)


def scan_body(chunk, *refs):
    refs = list(refs)
    heads = SIZES[chunk]
    count = STEPS[chunk]
    final_chunk = chunk == CHUNKS - 1
    me, owner, dl = refs[:3]
    per = 3 if final_chunk else 2
    held = [refs[3 + per * k : 3 + per * (k + 1)] for k in range(count)]
    refs = refs[3 + per * count :]
    b_ref, c_ref, xt, base, ecx = refs[:5]
    refs = refs[5:]
    prev = []
    if chunk > 0:
        prev = refs[1 : 1 + chunk]
        refs = refs[1 + chunk :]
    if final_chunk:
        gain, fin, out, proj = refs
    else:
        fin, gated_ref = refs
    i = pl.program_id(0)
    if final_chunk:
        states = [h[0][0] for h in held]
    else:
        states = [jnp.concatenate([h[0][0], h[1][0]], axis=0) for h in held]
    seen = jnp.concatenate(
        [
            lax.dot_general(
                c_ref[k * TAIL : (k + 1) * TAIL, :], states[k], NT, preferred_element_type=f32
            )
            for k in range(count)
        ],
        axis=0,
    )
    gated = base[...] + ecx[...] * seen
    if final_chunk:
        parts = [p[...] for p in prev] + [gated]
        energy = sum(jnp.sum(p * p, axis=1, keepdims=True) for p in parts)
        denom = jnp.sqrt(energy / WIDTH + 1e-5)
        for c in range(CHUNKS):
            cols = slice(STARTS[c] * HD, (STARTS[c] + SIZES[c]) * HD)
            out[:, cols] = (parts[c] / denom * gain[:, cols]).astype(bf16)
        for k in range(count):
            upper = (owner[me[0] * REQ + count * i + k] & 1) == 1
            for c in range(4):
                slab = held[k][1 + c % 2]
                at = (c // 2) * TAIL
                proj[k * TAIL : (k + 1) * TAIL, c * DH : (c + 1) * DH] = jnp.where(
                    upper,
                    slab[0, 2 * TAIL + at : 3 * TAIL + at, :],
                    slab[0, at : TAIL + at, :],
                )
    else:
        gated_ref[...] = gated
    who = lax.broadcasted_iota(jnp.int32, (128, STATE), 0) // TAIL
    rows = b_ref[...].astype(f32)
    at = (count * i) & 7
    mine = jnp.concatenate(
        [jnp.where(who == at + k, rows, 0.0).astype(bf16) for k in range(count)], axis=1
    )
    update = dot(xt[0], jnp.concatenate([mine, mine], axis=0))
    for k in range(count):
        for e in range(heads):
            rr = slice(e * HD, (e + 1) * HD)
            fin[k, e] = (
                dl[count * i + k, STARTS[chunk] + e] * states[k][rr].astype(f32)
                + update[rr, k * STATE : (k + 1) * STATE]
            ).astype(bf16)


def scan(chunk, me, owner, dl, got, b, c, xt, base, ecx, fin, prev, gain):
    final_chunk = chunk == CHUNKS - 1
    heads = SIZES[chunk]
    count = STEPS[chunk]
    width = heads * HD
    at = STARTS[chunk] // heads
    rows = count * TAIL

    def who(i, m, o, k):
        return o[m[0] * REQ + count * i + k]

    def held(k):
        if final_chunk:
            return [
                pl.BlockSpec((1, LAST, STATE), lambda i, m, o: (who(i, m, o, k), 0, 0)),
                pl.BlockSpec(
                    (1, SLAB, STATE), lambda i, m, o: (who(i, m, o, k) // 2 * 2, LAST // SLAB, 0)
                ),
                pl.BlockSpec(
                    (1, SLAB, STATE),
                    lambda i, m, o: (who(i, m, o, k) // 2 * 2 + 1, LAST // SLAB, 0),
                ),
            ]
        return [
            pl.BlockSpec((1, MOST, STATE), lambda i, m, o: (who(i, m, o, k), 0, 0)),
            pl.BlockSpec((1, EARLY, STATE), lambda i, m, o: (who(i, m, o, k), 0, 0)),
        ]

    def span(w, col=0):
        return pl.BlockSpec((rows, w), lambda i, m, o: (i, col))

    in_specs = [SMEM] + [spec for k in range(count) for spec in held(k)]
    in_specs += [
        pl.BlockSpec((128, STATE), lambda i, m, o: (i * count // 8, 0)),
        span(STATE),
        pl.BlockSpec((1, width, 256), lambda i, m, o: (i * count // 8, at, 0)),
        span(width, at),
        span(width, at),
    ]
    args = [dl] + list(got) * count + [b, c, xt, base, ecx]
    alias = {}
    if chunk > 0:
        alias = {2 + len(args): 0}
        in_specs += [ANY] + [span(p.shape[1]) for p in prev]
        args += [fin] + prev
    out_specs = [pl.BlockSpec((count, heads, HD, STATE), lambda i, m, o: (i, at, 0, 0))]
    out_shape = [sds((REQ, HEADS, HD, STATE), bf16)]
    if final_chunk:
        in_specs.append(pl.BlockSpec((1, WIDTH), lambda i, m, o: (0, 0)))
        args.append(gain)
        out_specs += [span(WIDTH), span(4 * DH)]
        out_shape += [sds((TOK, WIDTH), bf16), sds((TOK, 4 * DH), bf16)]
    else:
        out_specs += [span(width)]
        out_shape += [sds((TOK, width), f32)]

    def body(*refs):
        scan_body(chunk, *refs)

    return pl.pallas_call(
        body,
        grid_spec=pltpu.PrefetchScalarGridSpec(
            num_scalar_prefetch=2,
            grid=(REQ // count,),
            in_specs=in_specs,
            out_specs=out_specs,
        ),
        out_shape=out_shape,
        input_output_aliases=alias,
        compiler_params=params(dimension_semantics=("arbitrary",)),
        cost_estimate=pl.CostEstimate(
            flops=4_000_000_000, transcendentals=0, bytes_accessed=8_000_000
        ),
    )(me, owner, *args)


def exchange(x, axis):
    return lax.all_to_all(x, axis, split_axis=0, concat_axis=0, tiled=True)


def place(x, y, core):
    return (x & 3) * 8 + (y & 3) * 2 + core


def hop(v, axis, by):
    dx, dy = (by, 0) if axis == "x" else (0, by)
    pairs = [
        (place(x, y, c), place(x + dx, y + dy, c))
        for x in range(4)
        for y in range(4)
        for c in range(2)
    ]
    return lax.ppermute(v, "rep", pairs)


def ring(v, axis):
    return jnp.stack([v, hop(v, axis, 1), hop(v, axis, -1), hop(v, axis, 2)])


def sides(v, axis):
    return hop(v, axis, 1), hop(v, axis, -1)


def across(v, axis, left, right):
    n = v.shape[0] // 2
    return v, left, right, hop(right[:n], axis, -1), hop(left[n:], axis, 1)


def turn(v, by):
    return lax.ppermute(v, "head", [(z, (z + by) % NHEAD) for z in range(NHEAD)])


def step(
    ssd_x,
    gate_z,
    group_b,
    group_c,
    step_dt,
    queries,
    tail_kv,
    ckpt_state,
    kv_pool,
    w_out,
    decay_rate,
    skip_d,
    norm_gain,
    owner,
    slot,
    page_table,
    hit_len,
    tail_len,
):
    me = lax.axis_index("rep").astype(jnp.int32).reshape(1)
    head = lax.axis_index("head").astype(jnp.int32).reshape(1)
    swap = [(r, r ^ 1) for r in range(REPS)]
    half = w_out.shape[0] // 2
    ckpt = ckpt_state.reshape(REQ, WIDTH, STATE)
    queued, req = pack_first(me, owner, slot, queries, tail_kv, ckpt)
    asked = exchange(queued, "rep")
    a_half = ring(w_out[:half], "x")
    b_half = ring(w_out[half:], "y")
    a_side = sides(a_half, "y")
    b_side = sides(b_half, "x")
    a_ring = across(a_half, "y", *a_side)
    b_ring = across(b_half, "x", *b_side)
    most, packed, both = pack_s(me, owner, slot, req, ckpt)
    most = lax.optimization_barrier((most, asked, a_ring[3], a_ring[4], b_ring[3], b_ring[4]))[0]
    got = exchange(most, "rep")
    attn = attend(req, page_table.reshape(-1), hit_len, tail_len, asked, kv_pool)
    other = lax.ppermute(attn, "rep", swap)
    terms = project(me, head, attn, other, a_ring, b_ring)
    one, three, seven, five = relay(terms, turn(terms[0:6], 1), turn(terms[6:12], -1))
    parts = [turn(one, 1), turn(three, 3), turn(seven, -1), turn(five, -3)]
    base, ecx, xt, dl = prepare(
        me,
        tail_len,
        ssd_x,
        gate_z,
        group_b,
        group_c,
        step_dt,
        decay_rate.reshape(1, -1),
        skip_d.reshape(1, -1),
    )
    gain = norm_gain.reshape(1, -1)
    last = exchange(total(both, terms, parts, packed), "rep")
    fin, rows = scan(
        0, me, owner, dl, (got, asked), group_b, group_c, xt, base, ecx, None, [], gain
    )
    fin, out, projected = scan(
        1, me, owner, dl, (last,) * 3, group_b, group_c, xt, base, ecx, fin, [rows], gain
    )
    return out, projected, fin


def solution(mesh):
    return jax.shard_map(
        step,
        mesh=mesh,
        in_specs=(
            P("rep", "head"),
            P("rep", "head"),
            P("rep", "head"),
            P("rep", "head"),
            P("rep", "head"),
            P("rep", "head"),
            P("rep", "head"),
            P("rep", "head", None, None),
            P("rep", None, "head"),
            P("head", "rep"),
            P("head"),
            P("head"),
            P("head"),
            P(),
            P(),
            P(),
            P(),
            P(),
        ),
        out_specs=(P("rep", "head"), P("rep", "head"), P("rep", "head", None, None)),
        check_vma=False,
    )
```

```python
import math

import jax
import jax.numpy as jnp
from jax import lax
from jax.experimental import pallas as pl
from jax.experimental.pallas import tpu as pltpu
from jax.sharding import PartitionSpec as P


TAIL = 16
STATE = 128
QH = 8
DH = 128
REQ = 16
REPS = 32
HEADS = 16
HD = 64
PAGES = 16
CACHE = 256
TOK = REQ * TAIL
WIDTH = HEADS * HD
NHEAD = 8
NEAR = (0, -1, 1, 2)
SIZES = (12, 4)
STARTS = (0, 12)
STEPS = (2, 4)
CHUNKS = len(SIZES)
EARLY = 2 * HD
MOST = 10 * HD
LAST = 4 * HD
SLAB = 4 * TAIL
ASK = (QH + 2) * TAIL

f32 = jnp.float32
bf16 = jnp.bfloat16
SMEM = pl.BlockSpec(memory_space=pltpu.SMEM)
VMEM = pl.BlockSpec(memory_space=pltpu.VMEM)
ANY = pl.BlockSpec(memory_space=pl.ANY)
NT = (((1,), (1,)), ((), ()))


def dot(a, b):
    return jnp.dot(a, b, preferred_element_type=f32)


def split2(v):
    hi = v.astype(bf16)
    return hi, (v - hi.astype(f32)).astype(bf16)


def split3(v):
    hi = v.astype(bf16)
    rest = v - hi.astype(f32)
    mid = rest.astype(bf16)
    return hi, mid, (rest - mid.astype(f32)).astype(bf16)


def sds(shape, dtype):
    return jax.ShapeDtypeStruct(shape, dtype)


def params(**kw):
    return pltpu.CompilerParams(**kw)


def serve(owner, slot, mine, req, base):
    def home(h, carry):
        s = jnp.int32(0)
        g = jnp.int32(0)
        for j in range(REQ):
            hit = owner[h * REQ + j] == mine
            s = jnp.where(hit, slot[h * REQ + j] + 1, s)
            g = jnp.where(hit, h * REQ + j, g)

        @pl.when(s > 0)
        def _():
            req[base + s - 1] = g

        return carry

    lax.fori_loop(0, REPS, home, 0)


def pack_first_body(me, owner, slot, q, kv, ckpt, out, req, buf, tmp, come, go):
    for s in range(REQ):
        pltpu.make_async_copy(ckpt.at[s, pl.ds(MOST, EARLY)], buf.at[s], come.at[s]).start()
    first = me[0] * REQ
    for j in range(REQ):
        rows = slice(j * TAIL, (j + 1) * TAIL)
        for a in range(QH):
            tmp[j, a * TAIL : (a + 1) * TAIL, :] = q[rows, a * DH : (a + 1) * DH]
        for a in range(2):
            tmp[j, (QH + a) * TAIL : (QH + a + 1) * TAIL, :] = kv[rows, a * DH : (a + 1) * DH]
        pltpu.make_async_copy(
            tmp.at[j], out.at[owner[first + j], pl.ds(EARLY, ASK)], go.at[0]
        ).start()
    serve(owner, slot, me[0], req, 0)
    for s in range(REQ):
        pltpu.make_async_copy(ckpt.at[s, pl.ds(MOST, EARLY)], buf.at[s], come.at[s]).wait()
        pltpu.make_async_copy(buf.at[s], out.at[req[s] // REQ, pl.ds(0, EARLY)], go.at[1]).start()
    pltpu.make_async_copy(tmp, tmp, go.at[0]).wait()
    pltpu.make_async_copy(buf, buf, go.at[1]).wait()


def pack_first(me, owner, slot, q, kv, ckpt):
    return pl.pallas_call(
        pack_first_body,
        out_shape=[sds((REPS, EARLY + ASK, STATE), bf16), sds((REQ,), jnp.int32)],
        in_specs=[SMEM, SMEM, SMEM, VMEM, VMEM, ANY],
        out_specs=[ANY, SMEM],
        scratch_shapes=[
            pltpu.VMEM((REQ, EARLY, STATE), bf16),
            pltpu.VMEM((REQ, ASK, DH), bf16),
            pltpu.SemaphoreType.DMA((REQ,)),
            pltpu.SemaphoreType.DMA((2,)),
        ],
        name="pack_first",
    )(me, owner, slot, q, kv, ckpt)


def pack_s_body(me, owner, slot, req, ckpt, most, last, both, buf, come, go):
    for s in range(REQ):
        pltpu.make_async_copy(ckpt.at[s], buf.at[s], come.at[s]).start()
    for s in range(REQ):
        pltpu.make_async_copy(ckpt.at[s], buf.at[s], come.at[s]).wait()
        home = req[s] // REQ
        pltpu.make_async_copy(buf.at[s, pl.ds(0, MOST)], most.at[home], go.at[0]).start()
        pltpu.make_async_copy(
            buf.at[s, pl.ds(MOST + EARLY, LAST)], last.at[home, pl.ds(0, LAST)], go.at[1]
        ).start()
    par = me[0] & 1
    for s in range(REQ):
        both[par * REQ + s] = req[s]
    serve(owner, slot, me[0] + 1 - 2 * par, both, (1 - par) * REQ)
    for k, part in enumerate((buf.at[:, pl.ds(0, MOST)], buf.at[:, pl.ds(MOST + EARLY, LAST)])):
        pltpu.make_async_copy(part, part, go.at[k]).wait()


def pack_s(me, owner, slot, req, ckpt):
    return pl.pallas_call(
        pack_s_body,
        out_shape=[
            sds((REPS, MOST, STATE), bf16),
            sds((REPS, LAST + SLAB, STATE), bf16),
            sds((2 * REQ,), jnp.int32),
        ],
        in_specs=[SMEM, SMEM, SMEM, SMEM, ANY],
        out_specs=[ANY, ANY, SMEM],
        scratch_shapes=[
            pltpu.VMEM((REQ, WIDTH, STATE), bf16),
            pltpu.SemaphoreType.DMA((REQ,)),
            pltpu.SemaphoreType.DMA((2,)),
        ],
        name="pack_s",
    )(me, owner, slot, req, ckpt)


def attend_body(req, pages, hit, tail, qin, pool, out):
    row = lax.broadcasted_iota(jnp.int32, (QH * TAIL, CACHE + DH), 0) & (TAIL - 1)
    col = lax.broadcasted_iota(jnp.int32, (QH * TAIL, CACHE + DH), 1)
    late = col - CACHE
    causal = (late >= 0) & (late <= row)
    time = lax.broadcasted_iota(jnp.int32, (QH * TAIL, DH), 0) & (TAIL - 1)
    pad = jnp.zeros((DH - TAIL, DH), bf16)
    scale = 1.0 / math.sqrt(DH)

    def one(s, carry):
        g = req[s]
        ask = qin[g // REQ]
        rows = ask[EARLY : EARLY + QH * TAIL]
        held = [pool[pages[g * PAGES + i]] for i in range(PAGES)]
        keys = jnp.concatenate(
            [p[:, :DH] for p in held] + [ask[EARLY + ASK - 2 * TAIL : EARLY + ASK - TAIL], pad], axis=0
        )
        vals = jnp.concatenate([p[:, DH:] for p in held] + [ask[EARLY + ASK - TAIL :], pad], axis=0)
        scores = lax.dot_general(rows, keys, NT, preferred_element_type=f32) * scale
        visible = (col < hit[g]) | (causal & (late < tail[g]))
        scores = jnp.where(visible, scores, -1e30)
        top = jnp.max(scores, axis=1, keepdims=True)
        expo = jnp.where(visible, jnp.exp(scores - top), 0.0)
        weights = (expo / jnp.sum(expo, axis=1, keepdims=True)).astype(bf16)
        res = dot(weights, vals)
        res = jnp.where(time < tail[g], res, 0.0).astype(bf16)
        for a in range(QH):
            out[pl.ds(pl.multiple_of(s * TAIL, TAIL), TAIL), a * DH : (a + 1) * DH] = res[
                a * TAIL : (a + 1) * TAIL
            ]
        return carry

    lax.fori_loop(0, REQ, one, 0, unroll=2)


def attend(req, pages, hit, tail, qin, pool):
    return pl.pallas_call(
        attend_body,
        out_shape=sds((TOK, QH * DH), bf16),
        in_specs=[SMEM, SMEM, SMEM, SMEM, VMEM, VMEM],
        out_specs=VMEM,
        cost_estimate=pl.CostEstimate(
            flops=8_000_000_000, transcendentals=0, bytes_accessed=4_000_000
        ),
        name="attend",
    )(req, pages, hit, tail, qin, pool)


def spot(k, i):
    base = jnp.int32(12)
    for dist, start in ((1, 16), (2, 0), (3, 20), (5, 28), (6, 6), (7, 24)):
        base = jnp.where(k == dist, start, base)
    base = jnp.where(k == 4, jnp.where(i < 2, 4, 8), base)
    return base + i


def project_body(me, head, mine, other, *rest):
    a_ring, b_ring, out = rest[:8], rest[8:16], rest[16]
    x = me[0] // 8
    y = (me[0] // 2) & 3
    par = me[0] & 1
    half = QH * DH // 2

    def block(ring, outer, inner):
        return ring[2 * outer + inner // 2][inner % 2]

    for dy in range(4):
        for dx in (0, 2):
            top = jnp.concatenate([block(a_ring, dy, dx), block(a_ring, dy, dx + 1)], axis=1)
            low = jnp.concatenate([block(b_ring, dx, dy), block(b_ring, dx + 1, dy)], axis=1)
            for attn, core in ((mine, par), (other, 1 - par)):
                res = (dot(attn[:, :half], top) + dot(attn[:, half:], low)).astype(bf16)
                for k in range(2):
                    pair = ((x + NEAR[dx + k]) & 3) * 4 + ((y + NEAR[dy]) & 3)
                    dist = ((pair // 2) - head[0]) & (NHEAD - 1)
                    out[spot(dist, 2 * (pair & 1) + core)] = res[:, k * DH : (k + 1) * DH]


def project(me, head, mine, other, a_ring, b_ring):
    return pl.pallas_call(
        project_body,
        out_shape=sds((4 * NHEAD, TOK, DH), bf16),
        in_specs=[SMEM, SMEM] + [VMEM] * 18,
        out_specs=VMEM,
        cost_estimate=pl.CostEstimate(
            flops=8_000_000_000, transcendentals=0, bytes_accessed=11_000_000
        ),
        name="project",
    )(me, head, mine, other, *a_ring, *b_ring)


def relay_body(terms, up, down, one, three, seven, five):
    def add(a, b):
        return (a.astype(f32) + b.astype(f32)).astype(bf16)

    one[...] = add(terms[16:20], up[0:4])
    three[0:2] = add(terms[20:22], up[4:6])
    three[2:4] = terms[22:24]
    seven[...] = add(terms[24:28], down[0:4])
    five[0:2] = terms[28:30]
    five[2:4] = add(terms[30:32], down[4:6])


def relay(terms, up, down):
    return pl.pallas_call(
        relay_body,
        out_shape=[sds((4, TOK, DH), bf16)] * 4,
        in_specs=[VMEM] * 3,
        out_specs=[VMEM] * 4,
        cost_estimate=pl.CostEstimate(
            flops=1_000_000_000, transcendentals=0, bytes_accessed=3_000_000
        ),
        name="relay",
    )(terms, up, down)


def total_body(both, terms, *rest):
    parts = rest[:4]
    out, tmp, sem = rest[5:]
    for u in range(4):
        acc = terms[12 + u].astype(f32)
        for p in parts:
            acc = acc + p[u].astype(f32)
        acc = acc.astype(bf16)
        i, core = u // 2, u % 2
        for s in range(REQ):
            tmp[core * REQ + s, i * TAIL : (i + 1) * TAIL, :] = acc[s * TAIL : (s + 1) * TAIL]
    for s in range(2 * REQ):
        at = LAST + (s // REQ) * 2 * TAIL
        pltpu.make_async_copy(
            tmp.at[s], out.at[both[s] // REQ, pl.ds(at, 2 * TAIL)], sem.at[0]
        ).start()
    pltpu.make_async_copy(tmp, tmp, sem.at[0]).wait()


def total(both, terms, parts, packed):
    return pl.pallas_call(
        total_body,
        out_shape=sds(packed.shape, bf16),
        in_specs=[SMEM] + [VMEM] * 5 + [ANY],
        out_specs=ANY,
        input_output_aliases={6: 0},
        scratch_shapes=[pltpu.VMEM((2 * REQ, 2 * TAIL, DH), bf16), pltpu.SemaphoreType.DMA((1,))],
        cost_estimate=pl.CostEstimate(
            flops=1_000_000_000, transcendentals=0, bytes_accessed=3_000_000
        ),
        name="total",
    )(both, terms, *parts, packed)


def prepare_body(
    me, tail, x_ref, z_ref, b_ref, c_ref, dt_ref, rate, skip, base_ref, ecx_ref, xt_ref, dl_ref, tmp
):
    first = me[0] * REQ
    req16 = lax.broadcasted_iota(jnp.int32, (TOK, HEADS), 0) // TAIL
    tim16 = lax.broadcasted_iota(jnp.int32, (TOK, HEADS), 0) & (TAIL - 1)
    limit = jnp.zeros((TOK, HEADS), jnp.int32)
    for j in range(REQ):
        limit = jnp.where(req16 == j, tail[first + j], limit)
    live = (tim16 < limit).astype(f32)
    wdt = dt_ref[...].astype(f32) * live
    decay = -rate[...] * wdt
    r = lax.broadcasted_iota(jnp.int32, (TOK, TOK), 0)
    u = lax.broadcasted_iota(jnp.int32, (TOK, TOK), 1)
    same = (r // TAIL) == (u // TAIL)
    tri = same & (u <= r)
    trib = tri.astype(f32).astype(bf16)
    allb = same.astype(f32).astype(bf16)
    pieces = split3(decay)
    cum = dot(trib, pieces[0]) + dot(trib, pieces[1]) + dot(trib, pieces[2])
    last = dot(allb, pieces[0]) + dot(allb, pieces[1]) + dot(allb, pieces[2])
    tmp[...] = jnp.exp(last)
    dl_ref[...] = tmp[pl.ds(0, REQ, stride=TAIL), :]
    er = lax.broadcasted_iota(jnp.int32, (HEADS, WIDTH), 0)
    ec = lax.broadcasted_iota(jnp.int32, (HEADS, WIDTH), 1)
    onehot = ((ec // HD) == er).astype(f32).astype(bf16)

    def widen(v):
        a, b, c = split3(v)
        return dot(a, onehot) + dot(b, onehot) + dot(c, onehot)

    x = x_ref[...].astype(f32)
    hi, lo = split2(widen(jnp.exp(-cum) * wdt) * x)
    cb = jnp.where(
        tri, lax.dot_general(c_ref[...], b_ref[...], NT, preferred_element_type=f32), 0.0
    )
    chi, clo = split2(cb)
    within = dot(chi, hi) + dot(chi, lo) + dot(clo, hi)
    z = z_ref[...].astype(f32)
    gate = z / (1.0 + jnp.exp(-z))
    ecx = widen(jnp.exp(cum) * live)
    base_ref[...] = (ecx * within + widen(skip[...] * live) * x) * gate
    ecx_ref[...] = ecx * gate
    hi, lo = split2(widen(jnp.exp(last - cum) * wdt) * x)
    for k in range(2):
        rows = slice(k * 128, (k + 1) * 128)
        xt_ref[k, :, :128] = hi[rows].T
        xt_ref[k, :, 128:] = lo[rows].T


def prepare(me, tail, x, z, b, c, dt, rate, skip):
    return pl.pallas_call(
        prepare_body,
        out_shape=[
            sds((TOK, WIDTH), f32),
            sds((TOK, WIDTH), f32),
            sds((2, WIDTH, 256), bf16),
            sds((REQ, HEADS), f32),
        ],
        in_specs=[SMEM, SMEM] + [VMEM] * 7,
        out_specs=[VMEM] * 4,
        scratch_shapes=[pltpu.VMEM((TOK, HEADS), f32)],
        cost_estimate=pl.CostEstimate(
            flops=8_000_000_000, transcendentals=0, bytes_accessed=5_000_000
        ),
        name="prepare",
    )(me, tail, x, z, b, c, dt, rate, skip)


def scan_body(chunk, *refs):
    refs = list(refs)
    heads = SIZES[chunk]
    count = STEPS[chunk]
    final_chunk = chunk == CHUNKS - 1
    me, owner, dl = refs[:3]
    per = 3 if final_chunk else 2
    held = [refs[3 + per * k : 3 + per * (k + 1)] for k in range(count)]
    refs = refs[3 + per * count :]
    b_ref, c_ref, xt, base, ecx = refs[:5]
    refs = refs[5:]
    prev = []
    if chunk > 0:
        prev = refs[1 : 1 + chunk]
        refs = refs[1 + chunk :]
    if final_chunk:
        gain, fin, out, proj = refs
    else:
        fin, gated_ref = refs
    i = pl.program_id(0)
    if final_chunk:
        states = [h[0][0] for h in held]
    else:
        states = [jnp.concatenate([h[0][0], h[1][0]], axis=0) for h in held]
    seen = jnp.concatenate(
        [
            lax.dot_general(
                c_ref[k * TAIL : (k + 1) * TAIL, :], states[k], NT, preferred_element_type=f32
            )
            for k in range(count)
        ],
        axis=0,
    )
    gated = base[...] + ecx[...] * seen
    if final_chunk:
        parts = [p[...] for p in prev] + [gated]
        energy = sum(jnp.sum(p * p, axis=1, keepdims=True) for p in parts)
        denom = jnp.sqrt(energy / WIDTH + 1e-5)
        for c in range(CHUNKS):
            cols = slice(STARTS[c] * HD, (STARTS[c] + SIZES[c]) * HD)
            out[:, cols] = (parts[c] / denom * gain[:, cols]).astype(bf16)
        for k in range(count):
            upper = (owner[me[0] * REQ + count * i + k] & 1) == 1
            for c in range(4):
                slab = held[k][1 + c % 2]
                at = (c // 2) * TAIL
                proj[k * TAIL : (k + 1) * TAIL, c * DH : (c + 1) * DH] = jnp.where(
                    upper,
                    slab[0, 2 * TAIL + at : 3 * TAIL + at, :],
                    slab[0, at : TAIL + at, :],
                )
    else:
        gated_ref[...] = gated
    who = lax.broadcasted_iota(jnp.int32, (128, STATE), 0) // TAIL
    rows = b_ref[...].astype(f32)
    at = (count * i) & 7
    mine = jnp.concatenate(
        [jnp.where(who == at + k, rows, 0.0).astype(bf16) for k in range(count)], axis=1
    )
    update = dot(xt[0], jnp.concatenate([mine, mine], axis=0))
    for k in range(count):
        for e in range(heads):
            rr = slice(e * HD, (e + 1) * HD)
            fin[k, e] = (
                dl[count * i + k, STARTS[chunk] + e] * states[k][rr].astype(f32)
                + update[rr, k * STATE : (k + 1) * STATE]
            ).astype(bf16)


def scan(chunk, me, owner, dl, got, b, c, xt, base, ecx, fin, prev, gain):
    final_chunk = chunk == CHUNKS - 1
    heads = SIZES[chunk]
    count = STEPS[chunk]
    width = heads * HD
    at = STARTS[chunk] // heads
    rows = count * TAIL

    def who(i, m, o, k):
        return o[m[0] * REQ + count * i + k]

    def held(k):
        if final_chunk:
            return [
                pl.BlockSpec((1, LAST, STATE), lambda i, m, o: (who(i, m, o, k), 0, 0)),
                pl.BlockSpec(
                    (1, SLAB, STATE), lambda i, m, o: (who(i, m, o, k) // 2 * 2, LAST // SLAB, 0)
                ),
                pl.BlockSpec(
                    (1, SLAB, STATE),
                    lambda i, m, o: (who(i, m, o, k) // 2 * 2 + 1, LAST // SLAB, 0),
                ),
            ]
        return [
            pl.BlockSpec((1, MOST, STATE), lambda i, m, o: (who(i, m, o, k), 0, 0)),
            pl.BlockSpec((1, EARLY, STATE), lambda i, m, o: (who(i, m, o, k), 0, 0)),
        ]

    def span(w, col=0):
        return pl.BlockSpec((rows, w), lambda i, m, o: (i, col))

    in_specs = [SMEM] + [spec for k in range(count) for spec in held(k)]
    in_specs += [
        pl.BlockSpec((128, STATE), lambda i, m, o: (i * count // 8, 0)),
        span(STATE),
        pl.BlockSpec((1, width, 256), lambda i, m, o: (i * count // 8, at, 0)),
        span(width, at),
        span(width, at),
    ]
    args = [dl] + list(got) * count + [b, c, xt, base, ecx]
    alias = {}
    if chunk > 0:
        alias = {2 + len(args): 0}
        in_specs += [ANY] + [span(p.shape[1]) for p in prev]
        args += [fin] + prev
    out_specs = [pl.BlockSpec((count, heads, HD, STATE), lambda i, m, o: (i, at, 0, 0))]
    out_shape = [sds((REQ, HEADS, HD, STATE), bf16)]
    if final_chunk:
        in_specs.append(pl.BlockSpec((1, WIDTH), lambda i, m, o: (0, 0)))
        args.append(gain)
        out_specs += [span(WIDTH), span(4 * DH)]
        out_shape += [sds((TOK, WIDTH), bf16), sds((TOK, 4 * DH), bf16)]
    else:
        out_specs += [span(width)]
        out_shape += [sds((TOK, width), f32)]

    def body(*refs):
        scan_body(chunk, *refs)

    return pl.pallas_call(
        body,
        grid_spec=pltpu.PrefetchScalarGridSpec(
            num_scalar_prefetch=2,
            grid=(REQ // count,),
            in_specs=in_specs,
            out_specs=out_specs,
        ),
        out_shape=out_shape,
        input_output_aliases=alias,
        compiler_params=params(dimension_semantics=("arbitrary",)),
        cost_estimate=pl.CostEstimate(
            flops=4_000_000_000, transcendentals=0, bytes_accessed=8_000_000
        ),
    )(me, owner, *args)


def exchange(x, axis):
    return lax.all_to_all(x, axis, split_axis=0, concat_axis=0, tiled=True)


def place(x, y, core):
    return (x & 3) * 8 + (y & 3) * 2 + core


def hop(v, axis, by):
    dx, dy = (by, 0) if axis == "x" else (0, by)
    pairs = [
        (place(x, y, c), place(x + dx, y + dy, c))
        for x in range(4)
        for y in range(4)
        for c in range(2)
    ]
    return lax.ppermute(v, "rep", pairs)


def ring(v, axis):
    return (
        jnp.stack([v, hop(v, axis, 1)]),
        jnp.stack([hop(v, axis, -1), hop(v, axis, 2)]),
    )


def sides(v, axis):
    return [hop(p, axis, by) for by in (1, -1) for p in v]


def across(v, axis, near):
    return [*v, *near, hop(near[2], axis, -1), hop(near[1], axis, 1)]


def turn(v, by):
    return lax.ppermute(v, "head", [(z, (z + by) % NHEAD) for z in range(NHEAD)])


def step(
    ssd_x,
    gate_z,
    group_b,
    group_c,
    step_dt,
    queries,
    tail_kv,
    ckpt_state,
    kv_pool,
    w_out,
    decay_rate,
    skip_d,
    norm_gain,
    owner,
    slot,
    page_table,
    hit_len,
    tail_len,
):
    me = lax.axis_index("rep").astype(jnp.int32).reshape(1)
    head = lax.axis_index("head").astype(jnp.int32).reshape(1)
    swap = [(r, r ^ 1) for r in range(REPS)]
    half = w_out.shape[0] // 2
    ckpt = ckpt_state.reshape(REQ, WIDTH, STATE)
    queued, req = pack_first(me, owner, slot, queries, tail_kv, ckpt)
    asked = exchange(queued, "rep")
    a_half = ring(w_out[:half], "x")
    b_half = ring(w_out[half:], "y")
    a_side = sides(a_half, "y")
    b_side = sides(b_half, "x")
    a_ring = across(a_half, "y", a_side)
    b_ring = across(b_half, "x", b_side)
    most, packed, both = pack_s(me, owner, slot, req, ckpt)
    most = lax.optimization_barrier((most, asked))[0]
    got = exchange(most, "rep")
    attn = attend(req, page_table.reshape(-1), hit_len, tail_len, asked, kv_pool)
    other = lax.ppermute(attn, "rep", swap)
    terms = project(me, head, attn, other, a_ring, b_ring)
    one, three, seven, five = relay(terms, turn(terms[0:6], 1), turn(terms[6:12], -1))
    parts = [turn(one, 1), turn(three, 3), turn(seven, -1), turn(five, -3)]
    base, ecx, xt, dl = prepare(
        me,
        tail_len,
        ssd_x,
        gate_z,
        group_b,
        group_c,
        step_dt,
        decay_rate.reshape(1, -1),
        skip_d.reshape(1, -1),
    )
    gain = norm_gain.reshape(1, -1)
    last = exchange(total(both, terms, parts, packed), "rep")
    fin, rows = scan(
        0, me, owner, dl, (got, asked), group_b, group_c, xt, base, ecx, None, [], gain
    )
    fin, out, projected = scan(
        1, me, owner, dl, (last,) * 3, group_b, group_c, xt, base, ecx, fin, [rows], gain
    )
    return out, projected, fin


def solution(mesh):
    return jax.shard_map(
        step,
        mesh=mesh,
        in_specs=(
            P("rep", "head"),
            P("rep", "head"),
            P("rep", "head"),
            P("rep", "head"),
            P("rep", "head"),
            P("rep", "head"),
            P("rep", "head"),
            P("rep", "head", None, None),
            P("rep", None, "head"),
            P("head", "rep"),
            P("head"),
            P("head"),
            P("head"),
            P(),
            P(),
            P(),
            P(),
            P(),
        ),
        out_specs=(P("rep", "head"), P("rep", "head"), P("rep", "head", None, None)),
        check_vma=False,
    )
```

```python
import math

import jax
import jax.numpy as jnp
from jax import lax
from jax.experimental import pallas as pl
from jax.experimental.pallas import tpu as pltpu
from jax.sharding import PartitionSpec as P


TAIL = 16
STATE = 128
QH = 8
DH = 128
REQ = 16
REPS = 32
HEADS = 16
HD = 64
PAGES = 16
CACHE = 256
TOK = REQ * TAIL
WIDTH = HEADS * HD
NHEAD = 8
NEAR = (0, -1, 1, 2)
SIZES = (12, 4)
STARTS = (0, 12)
STEPS = (2, 4)
CHUNKS = len(SIZES)
EARLY = 2 * HD
MOST = 10 * HD
LAST = 4 * HD
SLAB = 4 * TAIL
ASK = (QH + 2) * TAIL

f32 = jnp.float32
bf16 = jnp.bfloat16
SMEM = pl.BlockSpec(memory_space=pltpu.SMEM)
VMEM = pl.BlockSpec(memory_space=pltpu.VMEM)
ANY = pl.BlockSpec(memory_space=pl.ANY)
NT = (((1,), (1,)), ((), ()))


def dot(a, b):
    return jnp.dot(a, b, preferred_element_type=f32)


def split2(v):
    hi = v.astype(bf16)
    return hi, (v - hi.astype(f32)).astype(bf16)


def split3(v):
    hi = v.astype(bf16)
    rest = v - hi.astype(f32)
    mid = rest.astype(bf16)
    return hi, mid, (rest - mid.astype(f32)).astype(bf16)


def sds(shape, dtype):
    return jax.ShapeDtypeStruct(shape, dtype)


def params(**kw):
    return pltpu.CompilerParams(**kw)


def serve(owner, slot, mine, req, base):
    def home(h, carry):
        s = jnp.int32(0)
        g = jnp.int32(0)
        for j in range(REQ):
            hit = owner[h * REQ + j] == mine
            s = jnp.where(hit, slot[h * REQ + j] + 1, s)
            g = jnp.where(hit, h * REQ + j, g)

        @pl.when(s > 0)
        def _():
            req[base + s - 1] = g

        return carry

    lax.fori_loop(0, REPS, home, 0)


def pack_first_body(me, owner, slot, q, kv, ckpt, out, req, buf, tmp, come, go):
    for s in range(REQ):
        pltpu.make_async_copy(ckpt.at[s, pl.ds(MOST, EARLY)], buf.at[s], come.at[s]).start()
    first = me[0] * REQ
    for j in range(REQ):
        rows = slice(j * TAIL, (j + 1) * TAIL)
        for a in range(QH):
            tmp[j, a * TAIL : (a + 1) * TAIL, :] = q[rows, a * DH : (a + 1) * DH]
        for a in range(2):
            tmp[j, (QH + a) * TAIL : (QH + a + 1) * TAIL, :] = kv[rows, a * DH : (a + 1) * DH]
        pltpu.make_async_copy(
            tmp.at[j], out.at[owner[first + j], pl.ds(EARLY, ASK)], go.at[0]
        ).start()
    serve(owner, slot, me[0], req, 0)
    for s in range(REQ):
        pltpu.make_async_copy(ckpt.at[s, pl.ds(MOST, EARLY)], buf.at[s], come.at[s]).wait()
        pltpu.make_async_copy(buf.at[s], out.at[req[s] // REQ, pl.ds(0, EARLY)], go.at[1]).start()
    pltpu.make_async_copy(tmp, tmp, go.at[0]).wait()
    pltpu.make_async_copy(buf, buf, go.at[1]).wait()


def pack_first(me, owner, slot, q, kv, ckpt):
    return pl.pallas_call(
        pack_first_body,
        out_shape=[sds((REPS, EARLY + ASK, STATE), bf16), sds((REQ,), jnp.int32)],
        in_specs=[SMEM, SMEM, SMEM, VMEM, VMEM, ANY],
        out_specs=[ANY, SMEM],
        scratch_shapes=[
            pltpu.VMEM((REQ, EARLY, STATE), bf16),
            pltpu.VMEM((REQ, ASK, DH), bf16),
            pltpu.SemaphoreType.DMA((REQ,)),
            pltpu.SemaphoreType.DMA((2,)),
        ],
        name="pack_first",
    )(me, owner, slot, q, kv, ckpt)


def pack_s_body(me, owner, slot, req, ckpt, most, last, both, buf, come, go):
    for s in range(REQ):
        pltpu.make_async_copy(ckpt.at[s], buf.at[s], come.at[s]).start()
    for s in range(REQ):
        pltpu.make_async_copy(ckpt.at[s], buf.at[s], come.at[s]).wait()
        home = req[s] // REQ
        pltpu.make_async_copy(buf.at[s, pl.ds(0, MOST)], most.at[home], go.at[0]).start()
        pltpu.make_async_copy(
            buf.at[s, pl.ds(MOST + EARLY, LAST)], last.at[home, pl.ds(0, LAST)], go.at[1]
        ).start()
    par = me[0] & 1
    for s in range(REQ):
        both[par * REQ + s] = req[s]
    serve(owner, slot, me[0] + 1 - 2 * par, both, (1 - par) * REQ)
    for k, part in enumerate((buf.at[:, pl.ds(0, MOST)], buf.at[:, pl.ds(MOST + EARLY, LAST)])):
        pltpu.make_async_copy(part, part, go.at[k]).wait()


def pack_s(me, owner, slot, req, ckpt):
    return pl.pallas_call(
        pack_s_body,
        out_shape=[
            sds((REPS, MOST, STATE), bf16),
            sds((REPS, LAST + SLAB, STATE), bf16),
            sds((2 * REQ,), jnp.int32),
        ],
        in_specs=[SMEM, SMEM, SMEM, SMEM, ANY],
        out_specs=[ANY, ANY, SMEM],
        scratch_shapes=[
            pltpu.VMEM((REQ, WIDTH, STATE), bf16),
            pltpu.SemaphoreType.DMA((REQ,)),
            pltpu.SemaphoreType.DMA((2,)),
        ],
        name="pack_s",
    )(me, owner, slot, req, ckpt)


def attend_body(req, pages, hit, tail, qin, pool, out):
    row = lax.broadcasted_iota(jnp.int32, (QH * TAIL, CACHE + DH), 0) & (TAIL - 1)
    col = lax.broadcasted_iota(jnp.int32, (QH * TAIL, CACHE + DH), 1)
    late = col - CACHE
    causal = (late >= 0) & (late <= row)
    time = lax.broadcasted_iota(jnp.int32, (QH * TAIL, DH), 0) & (TAIL - 1)
    pad = jnp.zeros((DH - TAIL, DH), bf16)
    scale = 1.0 / math.sqrt(DH)

    def one(s, carry):
        g = req[s]
        ask = qin[g // REQ]
        rows = ask[EARLY : EARLY + QH * TAIL]
        held = [pool[pages[g * PAGES + i]] for i in range(PAGES)]
        keys = jnp.concatenate(
            [p[:, :DH] for p in held] + [ask[EARLY + ASK - 2 * TAIL : EARLY + ASK - TAIL], pad], axis=0
        )
        vals = jnp.concatenate([p[:, DH:] for p in held] + [ask[EARLY + ASK - TAIL :], pad], axis=0)
        scores = lax.dot_general(rows, keys, NT, preferred_element_type=f32) * scale
        visible = (col < hit[g]) | (causal & (late < tail[g]))
        scores = jnp.where(visible, scores, -1e30)
        top = jnp.max(scores, axis=1, keepdims=True)
        expo = jnp.where(visible, jnp.exp(scores - top), 0.0)
        weights = (expo / jnp.sum(expo, axis=1, keepdims=True)).astype(bf16)
        res = dot(weights, vals)
        res = jnp.where(time < tail[g], res, 0.0).astype(bf16)
        for a in range(QH):
            out[pl.ds(pl.multiple_of(s * TAIL, TAIL), TAIL), a * DH : (a + 1) * DH] = res[
                a * TAIL : (a + 1) * TAIL
            ]
        return carry

    lax.fori_loop(0, REQ, one, 0, unroll=2)


def attend(req, pages, hit, tail, qin, pool):
    return pl.pallas_call(
        attend_body,
        out_shape=sds((TOK, QH * DH), bf16),
        in_specs=[SMEM, SMEM, SMEM, SMEM, VMEM, VMEM],
        out_specs=VMEM,
        cost_estimate=pl.CostEstimate(
            flops=8_000_000_000, transcendentals=0, bytes_accessed=4_000_000
        ),
        name="attend",
    )(req, pages, hit, tail, qin, pool)


def spot(k, i):
    base = jnp.int32(12)
    for dist, start in ((1, 16), (2, 0), (3, 20), (5, 28), (6, 6), (7, 24)):
        base = jnp.where(k == dist, start, base)
    base = jnp.where(k == 4, jnp.where(i < 2, 4, 8), base)
    return base + i


def project_body(me, head, mine, other, *rest):
    a_ring, b_ring, out = rest[:8], rest[8:16], rest[16]
    x = me[0] // 8
    y = (me[0] // 2) & 3
    par = me[0] & 1
    half = QH * DH // 2

    def block(ring, outer, inner):
        return ring[2 * outer + inner // 2][inner % 2]

    for dy in range(4):
        for dx in (0, 2):
            top = jnp.concatenate([block(a_ring, dy, dx), block(a_ring, dy, dx + 1)], axis=1)
            low = jnp.concatenate([block(b_ring, dx, dy), block(b_ring, dx + 1, dy)], axis=1)
            for attn, core in ((mine, par), (other, 1 - par)):
                res = (dot(attn[:, :half], top) + dot(attn[:, half:], low)).astype(bf16)
                for k in range(2):
                    pair = ((x + NEAR[dx + k]) & 3) * 4 + ((y + NEAR[dy]) & 3)
                    dist = ((pair // 2) - head[0]) & (NHEAD - 1)
                    out[spot(dist, 2 * (pair & 1) + core)] = res[:, k * DH : (k + 1) * DH]


def project(me, head, mine, other, a_ring, b_ring):
    return pl.pallas_call(
        project_body,
        out_shape=sds((4 * NHEAD, TOK, DH), bf16),
        in_specs=[SMEM, SMEM] + [VMEM] * 18,
        out_specs=VMEM,
        cost_estimate=pl.CostEstimate(
            flops=8_000_000_000, transcendentals=0, bytes_accessed=11_000_000
        ),
        name="project",
    )(me, head, mine, other, *a_ring, *b_ring)


def relay_body(terms, up, down, one, three, seven, five):
    def add(a, b):
        return (a.astype(f32) + b.astype(f32)).astype(bf16)

    one[...] = add(terms[16:20], up[0:4])
    three[0:2] = add(terms[20:22], up[4:6])
    three[2:4] = terms[22:24]
    seven[...] = add(terms[24:28], down[0:4])
    five[0:2] = terms[28:30]
    five[2:4] = add(terms[30:32], down[4:6])


def relay(terms, up, down):
    return pl.pallas_call(
        relay_body,
        out_shape=[sds((4, TOK, DH), bf16)] * 4,
        in_specs=[VMEM] * 3,
        out_specs=[VMEM] * 4,
        cost_estimate=pl.CostEstimate(
            flops=1_000_000_000, transcendentals=0, bytes_accessed=3_000_000
        ),
        name="relay",
    )(terms, up, down)


def total_body(both, terms, *rest):
    parts = rest[:4]
    out, tmp, sem = rest[5:]
    for u in range(4):
        acc = terms[12 + u].astype(f32)
        for p in parts:
            acc = acc + p[u].astype(f32)
        acc = acc.astype(bf16)
        i, core = u // 2, u % 2
        for s in range(REQ):
            tmp[core * REQ + s, i * TAIL : (i + 1) * TAIL, :] = acc[s * TAIL : (s + 1) * TAIL]
    for s in range(2 * REQ):
        at = LAST + (s // REQ) * 2 * TAIL
        pltpu.make_async_copy(
            tmp.at[s], out.at[both[s] // REQ, pl.ds(at, 2 * TAIL)], sem.at[0]
        ).start()
    pltpu.make_async_copy(tmp, tmp, sem.at[0]).wait()


def total(both, terms, parts, packed):
    return pl.pallas_call(
        total_body,
        out_shape=sds(packed.shape, bf16),
        in_specs=[SMEM] + [VMEM] * 5 + [ANY],
        out_specs=ANY,
        input_output_aliases={6: 0},
        scratch_shapes=[pltpu.VMEM((2 * REQ, 2 * TAIL, DH), bf16), pltpu.SemaphoreType.DMA((1,))],
        cost_estimate=pl.CostEstimate(
            flops=1_000_000_000, transcendentals=0, bytes_accessed=3_000_000
        ),
        name="total",
    )(both, terms, *parts, packed)


def prepare_body(
    me, tail, x_ref, z_ref, b_ref, c_ref, dt_ref, rate, skip, base_ref, ecx_ref, xt_ref, dl_ref, tmp
):
    first = me[0] * REQ
    req16 = lax.broadcasted_iota(jnp.int32, (TOK, HEADS), 0) // TAIL
    tim16 = lax.broadcasted_iota(jnp.int32, (TOK, HEADS), 0) & (TAIL - 1)
    limit = jnp.zeros((TOK, HEADS), jnp.int32)
    for j in range(REQ):
        limit = jnp.where(req16 == j, tail[first + j], limit)
    live = (tim16 < limit).astype(f32)
    wdt = dt_ref[...].astype(f32) * live
    decay = -rate[...] * wdt
    r = lax.broadcasted_iota(jnp.int32, (TOK, TOK), 0)
    u = lax.broadcasted_iota(jnp.int32, (TOK, TOK), 1)
    same = (r // TAIL) == (u // TAIL)
    tri = same & (u <= r)
    trib = tri.astype(f32).astype(bf16)
    allb = same.astype(f32).astype(bf16)
    pieces = split3(decay)
    cum = dot(trib, pieces[0]) + dot(trib, pieces[1]) + dot(trib, pieces[2])
    last = dot(allb, pieces[0]) + dot(allb, pieces[1]) + dot(allb, pieces[2])
    tmp[...] = jnp.exp(last)
    dl_ref[...] = tmp[pl.ds(0, REQ, stride=TAIL), :]
    er = lax.broadcasted_iota(jnp.int32, (HEADS, WIDTH), 0)
    ec = lax.broadcasted_iota(jnp.int32, (HEADS, WIDTH), 1)
    onehot = ((ec // HD) == er).astype(f32).astype(bf16)

    def widen(v):
        a, b, c = split3(v)
        return dot(a, onehot) + dot(b, onehot) + dot(c, onehot)

    x = x_ref[...].astype(f32)
    hi, lo = split2(widen(jnp.exp(-cum) * wdt) * x)
    cb = jnp.where(
        tri, lax.dot_general(c_ref[...], b_ref[...], NT, preferred_element_type=f32), 0.0
    )
    chi, clo = split2(cb)
    within = dot(chi, hi) + dot(chi, lo) + dot(clo, hi)
    z = z_ref[...].astype(f32)
    gate = z / (1.0 + jnp.exp(-z))
    ecx = widen(jnp.exp(cum) * live)
    base_ref[...] = (ecx * within + widen(skip[...] * live) * x) * gate
    ecx_ref[...] = ecx * gate
    hi, lo = split2(widen(jnp.exp(last - cum) * wdt) * x)
    for k in range(2):
        rows = slice(k * 128, (k + 1) * 128)
        xt_ref[k, :, :128] = hi[rows].T
        xt_ref[k, :, 128:] = lo[rows].T


def prepare(me, tail, x, z, b, c, dt, rate, skip):
    return pl.pallas_call(
        prepare_body,
        out_shape=[
            sds((TOK, WIDTH), f32),
            sds((TOK, WIDTH), f32),
            sds((2, WIDTH, 256), bf16),
            sds((REQ, HEADS), f32),
        ],
        in_specs=[SMEM, SMEM] + [VMEM] * 7,
        out_specs=[VMEM] * 4,
        scratch_shapes=[pltpu.VMEM((TOK, HEADS), f32)],
        cost_estimate=pl.CostEstimate(
            flops=8_000_000_000, transcendentals=0, bytes_accessed=5_000_000
        ),
        name="prepare",
    )(me, tail, x, z, b, c, dt, rate, skip)


def scan_body(chunk, *refs):
    refs = list(refs)
    heads = SIZES[chunk]
    count = STEPS[chunk]
    final_chunk = chunk == CHUNKS - 1
    me, owner, dl = refs[:3]
    i = pl.program_id(0)
    if final_chunk:
        got = refs[3]
        refs = refs[4:]
    else:
        held = [refs[3 + 2 * k : 5 + 2 * k] for k in range(count)]
        refs = refs[3 + 2 * count :]
    b_ref, c_ref, xt, base, ecx = refs[:5]
    refs = refs[5:]
    prev = []
    if chunk > 0:
        prev = refs[1 : 1 + chunk]
        refs = refs[1 + chunk :]
    if final_chunk:
        gain, fin, out, proj = refs
    else:
        fin, gated_ref = refs
    if final_chunk:
        hosts = [owner[me[0] * REQ + count * i + k] for k in range(count)]
        states = [got[o, :LAST] for o in hosts]
    else:
        states = [jnp.concatenate([h[0][0], h[1][0]], axis=0) for h in held]
    seen = jnp.concatenate(
        [
            lax.dot_general(
                c_ref[k * TAIL : (k + 1) * TAIL, :], states[k], NT, preferred_element_type=f32
            )
            for k in range(count)
        ],
        axis=0,
    )
    gated = base[...] + ecx[...] * seen
    if final_chunk:
        parts = [p[...] for p in prev] + [gated]
        energy = sum(jnp.sum(p * p, axis=1, keepdims=True) for p in parts)
        denom = jnp.sqrt(energy / WIDTH + 1e-5)
        for c in range(CHUNKS):
            cols = slice(STARTS[c] * HD, (STARTS[c] + SIZES[c]) * HD)
            out[:, cols] = (parts[c] / denom * gain[:, cols]).astype(bf16)
        for k in range(count):
            slabs = [got[hosts[k] // 2 * 2 + c, LAST:] for c in range(2)]
            upper = (hosts[k] & 1) == 1
            for c in range(4):
                at = (c // 2) * TAIL
                proj[k * TAIL : (k + 1) * TAIL, c * DH : (c + 1) * DH] = jnp.where(
                    upper,
                    slabs[c % 2][2 * TAIL + at : 3 * TAIL + at],
                    slabs[c % 2][at : TAIL + at],
                )
    else:
        gated_ref[...] = gated
    who = lax.broadcasted_iota(jnp.int32, (128, STATE), 0) // TAIL
    rows = b_ref[...].astype(f32)
    at = (count * i) & 7
    mine = jnp.concatenate(
        [jnp.where(who == at + k, rows, 0.0).astype(bf16) for k in range(count)], axis=1
    )
    update = dot(xt[0], jnp.concatenate([mine, mine], axis=0))
    for k in range(count):
        for e in range(heads):
            rr = slice(e * HD, (e + 1) * HD)
            fin[k, e] = (
                dl[count * i + k, STARTS[chunk] + e] * states[k][rr].astype(f32)
                + update[rr, k * STATE : (k + 1) * STATE]
            ).astype(bf16)


def scan(chunk, me, owner, dl, got, b, c, xt, base, ecx, fin, prev, gain):
    final_chunk = chunk == CHUNKS - 1
    heads = SIZES[chunk]
    count = STEPS[chunk]
    width = heads * HD
    at = STARTS[chunk] // heads
    rows = count * TAIL

    def who(i, m, o, k):
        return o[m[0] * REQ + count * i + k]

    def held(k):
        return [
            pl.BlockSpec((1, MOST, STATE), lambda i, m, o: (who(i, m, o, k), 0, 0)),
            pl.BlockSpec((1, EARLY, STATE), lambda i, m, o: (who(i, m, o, k), 0, 0)),
        ]

    def span(w, col=0):
        return pl.BlockSpec((rows, w), lambda i, m, o: (i, col))

    in_specs = [SMEM]
    if final_chunk:
        in_specs.append(VMEM)
        args = [dl, got]
    else:
        in_specs += [spec for k in range(count) for spec in held(k)]
        args = [dl] + list(got) * count
    in_specs += [
        pl.BlockSpec((128, STATE), lambda i, m, o: (i * count // 8, 0)),
        span(STATE),
        pl.BlockSpec((1, width, 256), lambda i, m, o: (i * count // 8, at, 0)),
        span(width, at),
        span(width, at),
    ]
    args += [b, c, xt, base, ecx]
    alias = {}
    if chunk > 0:
        alias = {2 + len(args): 0}
        in_specs += [ANY] + [span(p.shape[1]) for p in prev]
        args += [fin] + prev
    out_specs = [pl.BlockSpec((count, heads, HD, STATE), lambda i, m, o: (i, at, 0, 0))]
    out_shape = [sds((REQ, HEADS, HD, STATE), bf16)]
    if final_chunk:
        in_specs.append(pl.BlockSpec((1, WIDTH), lambda i, m, o: (0, 0)))
        args.append(gain)
        out_specs += [span(WIDTH), span(4 * DH)]
        out_shape += [sds((TOK, WIDTH), bf16), sds((TOK, 4 * DH), bf16)]
    else:
        out_specs += [span(width)]
        out_shape += [sds((TOK, width), f32)]

    def body(*refs):
        scan_body(chunk, *refs)

    return pl.pallas_call(
        body,
        grid_spec=pltpu.PrefetchScalarGridSpec(
            num_scalar_prefetch=2,
            grid=(REQ // count,),
            in_specs=in_specs,
            out_specs=out_specs,
        ),
        out_shape=out_shape,
        input_output_aliases=alias,
        compiler_params=params(dimension_semantics=("arbitrary",)),
        cost_estimate=pl.CostEstimate(
            flops=4_000_000_000, transcendentals=0, bytes_accessed=8_000_000
        ),
    )(me, owner, *args)


def exchange(x, axis):
    return lax.all_to_all(x, axis, split_axis=0, concat_axis=0, tiled=True)


def place(x, y, core):
    return (x & 3) * 8 + (y & 3) * 2 + core


def hop(v, axis, by):
    dx, dy = (by, 0) if axis == "x" else (0, by)
    pairs = [
        (place(x, y, c), place(x + dx, y + dy, c))
        for x in range(4)
        for y in range(4)
        for c in range(2)
    ]
    return lax.ppermute(v, "rep", pairs)


def ring(v, axis):
    return (
        jnp.stack([v, hop(v, axis, 1)]),
        jnp.stack([hop(v, axis, -1), hop(v, axis, 2)]),
    )


def sides(v, axis):
    return [hop(p, axis, by) for by in (1, -1) for p in v]


def across(v, axis, near):
    return [*v, *near, hop(near[2], axis, -1), hop(near[1], axis, 1)]


def turn(v, by):
    return lax.ppermute(v, "head", [(z, (z + by) % NHEAD) for z in range(NHEAD)])


def step(
    ssd_x,
    gate_z,
    group_b,
    group_c,
    step_dt,
    queries,
    tail_kv,
    ckpt_state,
    kv_pool,
    w_out,
    decay_rate,
    skip_d,
    norm_gain,
    owner,
    slot,
    page_table,
    hit_len,
    tail_len,
):
    me = lax.axis_index("rep").astype(jnp.int32).reshape(1)
    head = lax.axis_index("head").astype(jnp.int32).reshape(1)
    swap = [(r, r ^ 1) for r in range(REPS)]
    half = w_out.shape[0] // 2
    ckpt = ckpt_state.reshape(REQ, WIDTH, STATE)
    queued, req = pack_first(me, owner, slot, queries, tail_kv, ckpt)
    asked = exchange(queued, "rep")
    a_half = ring(w_out[:half], "x")
    b_half = ring(w_out[half:], "y")
    a_side = sides(a_half, "y")
    b_side = sides(b_half, "x")
    a_ring = across(a_half, "y", a_side)
    b_ring = across(b_half, "x", b_side)
    most, packed, both = pack_s(me, owner, slot, req, ckpt)
    most = lax.optimization_barrier((most, asked))[0]
    got = exchange(most, "rep")
    attn = attend(req, page_table.reshape(-1), hit_len, tail_len, asked, kv_pool)
    other = lax.ppermute(attn, "rep", swap)
    terms = project(me, head, attn, other, a_ring, b_ring)
    one, three, seven, five = relay(terms, turn(terms[0:6], 1), turn(terms[6:12], -1))
    parts = [turn(one, 1), turn(three, 3), turn(seven, -1), turn(five, -3)]
    base, ecx, xt, dl = prepare(
        me,
        tail_len,
        ssd_x,
        gate_z,
        group_b,
        group_c,
        step_dt,
        decay_rate.reshape(1, -1),
        skip_d.reshape(1, -1),
    )
    gain = norm_gain.reshape(1, -1)
    last = exchange(total(both, terms, parts, packed), "rep")
    last = pltpu.with_memory_space_constraint(last, pltpu.VMEM)
    fin, rows = scan(
        0, me, owner, dl, (got, asked), group_b, group_c, xt, base, ecx, None, [], gain
    )
    fin, out, projected = scan(
        1, me, owner, dl, last, group_b, group_c, xt, base, ecx, fin, [rows], gain
    )
    return out, projected, fin


def solution(mesh):
    return jax.shard_map(
        step,
        mesh=mesh,
        in_specs=(
            P("rep", "head"),
            P("rep", "head"),
            P("rep", "head"),
            P("rep", "head"),
            P("rep", "head"),
            P("rep", "head"),
            P("rep", "head"),
            P("rep", "head", None, None),
            P("rep", None, "head"),
            P("head", "rep"),
            P("head"),
            P("head"),
            P("head"),
            P(),
            P(),
            P(),
            P(),
            P(),
        ),
        out_specs=(P("rep", "head"), P("rep", "head"), P("rep", "head", None, None)),
        check_vma=False,
    )
```
